32 devices in a mesh: north: 8 (over y, x, core), deep: 4 (over z).
Axes of the slice: x: 2, y: 2, z: 4, core: 2. Of those that a mesh axis runs over, the one named last changes fastest.
Arguments:
- forcing: float32 [2, 128, 128, 256], P(None, None, 'north', 'deep'), may hold values from -6 to 6
- symbol_x: float32 [128], replicated, may hold values from 0.3 to 3
- symbol_y: float32 [128], replicated, may hold values from 0.3 to 3
- symbol_z: float32 [256], replicated, may hold values from 0.3 to 3
Outputs:
- coefficients: float32 [2, 128, 128, 256], P(None, 'north', 'deep')
The draws below stay inside these ranges and needn't reach their ends.
All inputs are finite; a program needn't handle non-finite values.
Results may differ from the reference program's by a relative error of at most 0.000084.
Values sent between devices are 32-bit elements; how exact they have to be, the bound alone decides.
A program may use at most 64 MiB of HBM per device.

```python
import jax
import jax.numpy as jnp
from jax import lax

GRID_X = 128
GRID_Y = 128
GRID_Z = 256
FIELDS = 2


def block_levels(rng, shape, pieces, least, largest):
    level, own = 1.0, jax.random.fold_in(rng, 6)
    for axis_at, blocks in pieces:
        steps = jnp.exp(jax.random.uniform(jax.random.fold_in(own, axis_at), (blocks,), jnp.float32, least / len(pieces), largest / len(pieces)))
        level = level * jnp.repeat(steps, shape[axis_at] // blocks).reshape([-1 if axis == axis_at else 1 for axis in range(len(shape))])
    return level


def bell_draw(rng, shape, spread, bound, cuts=(), dtype=jnp.bfloat16):
    entries = jax.random.normal(rng, shape, jnp.float32) * spread
    if len(cuts) > 0:
        entries = block_levels(rng, shape, cuts, -0.22, 0.18) * entries
    return jnp.clip(entries, min=-bound, max=bound).astype(dtype)


def setup_inputs(seed: int = 0) -> dict:
    splits = jax.random.split(jax.random.key(seed), 5)
    return {
        "forcing": bell_draw(splits[0], (FIELDS, GRID_X, GRID_Y, GRID_Z), 1.0, 6.0, ((2, 8), (3, 4)), jnp.float32),
        "symbol_x": jnp.clip(jax.random.uniform(splits[1], (GRID_X,), jnp.float32, 0.3, 3.0), 0.3, 3.0),
        "symbol_y": jnp.clip(jax.random.uniform(splits[2], (GRID_Y,), jnp.float32, 0.3, 3.0), 0.3, 3.0),
        "symbol_z": jnp.clip(jax.random.uniform(splits[3], (GRID_Z,), jnp.float32, 0.3, 3.0), 0.3, 3.0),
    }


def transform_table(count):
    rank = jnp.arange(count)
    angle = (jnp.pi / (4 * count)) * (((2 * rank[:, None] + 1) * (2 * rank[None, :] + 1)) % (8 * count)).astype(jnp.float32)
    return jnp.cos(angle) * (2.0 / count) ** 0.5


def to_modes(values, dim):
    moved = jnp.tensordot(values, transform_table(values.shape[dim]), axes=([dim], [0]), precision=lax.Precision.HIGHEST)
    return jnp.moveaxis(moved, -1, dim)


def reference(forcing, symbol_x, symbol_y, symbol_z):
    coefficients = forcing
    coefficients = to_modes(coefficients, 1)
    coefficients = to_modes(coefficients, 2)
    coefficients = to_modes(coefficients, 3)
    symbol = symbol_x[:, None, None] + symbol_y[None, :, None] + symbol_z[None, None, :]
    coefficients = coefficients * ((1.0 - 0.2 * symbol) / (1.0 + 0.2 * symbol))
    return coefficients
```

```python
import functools
import math

import jax
import jax.numpy as jnp
import numpy as np
from jax import lax
from jax.experimental import pallas as pl
from jax.experimental.pallas import tpu as pltpu
from jax.sharding import PartitionSpec as P

CHUNKS = (1, 1, 2, 4, 4, 3, 1)
EARLY = 2


def transform_table(count):
    rank = np.arange(count)
    odd = (2 * rank[:, None] + 1) * (2 * rank[None, :] + 1) % (8 * count)
    return (np.cos(np.pi / (4 * count) * odd) * np.sqrt(2.0 / count)).astype(np.float32)


def chunk_starts(share):
    unit = max(1, share // sum(CHUNKS))
    found, start = [], 0
    for weight in CHUNKS:
        size = min(unit * weight, share - start)
        if size > 0:
            found.append((start, size))
        start += size
    if start < share:
        found.append((start, share - start))
    return tuple(found)


def halves(values):
    high = values.astype(jnp.bfloat16)
    low = (values - high.astype(jnp.float32)).astype(jnp.bfloat16)
    return high, low


def table_halves(table):
    high = table.astype(jnp.bfloat16)
    low = (table - high.astype(np.float32)).astype(jnp.bfloat16)
    return high, low


def partners(me, count):
    found = []
    for step in range(count - 1, 0, -1):
        if count & (count - 1):
            found.append(lax.rem(me + step, count))
            continue
        other = me
        for bit in range(count.bit_length() - 1):
            if step >> bit & 1:
                other = other + (1 - 2 * ((me // 2**bit) % 2)) * 2**bit
        found.append(other)
    return found


def kernel(
    sizes, forcing, tx, ty, tz, gx, gy, gz, out, symbols, xin, hx, hy, hz, wa, u, v, r, fac,
    in_sem, table_sem, ns_sem, nr_sem, ds_sem, dr_sem,
):
    north, deep, chunks, early = sizes
    fields, share_y, share_z, grid_x = forcing.shape
    share_x, part_y = out.shape[1], out.shape[2]
    grid_y, grid_z = v.shape[1], out.shape[3]
    lanes = fields * share_z
    n, d = lax.axis_index("north"), lax.axis_index("deep")
    norths, deeps = partners(n, north), partners(d, deep)
    deeps = deeps[1:] + deeps[:1]

    barrier = pltpu.get_barrier_semaphore()
    for other in deeps:
        pl.semaphore_signal(barrier, device_id={"deep": other}, device_id_type=pl.DeviceIdType.MESH)
    for other in norths:
        pl.semaphore_signal(barrier, device_id={"north": other}, device_id_type=pl.DeviceIdType.MESH)

    first = pltpu.make_async_copy(tx, hx, table_sem.at[0])
    first.start()
    groups = in_sem.shape[0]
    per = share_y // groups
    loads = []
    for g in range(groups):
        part = (slice(None), pl.ds(g * per, per))
        loads.append(pltpu.make_async_copy(forcing.at[part], xin.at[part], in_sem.at[g]))
        loads[-1].start()
    tables = [pltpu.make_async_copy(source, target, table_sem.at[k + 1]) for k, (source, target) in enumerate(((ty, hy), (tz, hz)))]
    for table in tables:
        table.start()
    at = 0
    for source in (gx, gy, gz):
        span = pl.ds(at, source.shape[1])
        pltpu.make_async_copy(source, symbols.at[:, span], table_sem.at[3]).start()
        at += source.shape[1]

    pair = 2 if per % 2 == 0 else 1

    def along_x(g, start, count):
        for y in range(g * per, (g + 1) * per, pair):
            high, low = halves(
                jnp.concatenate([xin[f, y + k] for k in range(pair) for f in range(fields)], axis=0)
            )
            modes = lax.dot_general(
                hx[pl.ds(start, count), :],
                jnp.concatenate([high, low, high], axis=1),
                (((1,), (1,)), ((), ())),
                preferred_element_type=jnp.float32,
            )
            for k in range(pair):
                wa[pl.ds(start * share_y + y + k, count, stride=share_y), :] = modes[
                    :, k * lanes : (k + 1) * lanes
                ]

    def rows(c, other):
        start, size = chunks[c]
        at = (start * north + other * size) * share_y
        return pl.ds(pl.multiple_of(at, share_y), size * share_y)

    def north_copy(c, target, source):
        return pltpu.make_async_remote_copy(
            src_ref=wa.at[rows(c, target)],
            dst_ref=u.at[rows(c, source)],
            send_sem=ns_sem.at[0],
            recv_sem=nr_sem.at[c],
            device_id={"north": target},
            device_id_type=pl.DeviceIdType.MESH,
        )

    def north_landed(c):
        every = u.at[pl.ds(0, (north - 1) * chunks[c][1] * share_y)]
        pltpu.make_async_copy(every, every, nr_sem.at[c]).wait()

    def deep_copy(c, target, source):
        return pltpu.make_async_remote_copy(
            src_ref=v.at[pl.ds(*chunks[c]), pl.ds(pl.multiple_of(target * part_y, part_y), part_y)],
            dst_ref=r.at[source, pl.ds(*chunks[c])],
            send_sem=ds_sem.at[0],
            recv_sem=dr_sem.at[c],
            device_id={"deep": target},
            device_id_type=pl.DeviceIdType.MESH,
        )

    def deep_landed(c):
        every = r.at[pl.ds(0, deep - 1), pl.ds(0, chunks[c][1])]
        pltpu.make_async_copy(every, every, dr_sem.at[c]).wait()

    def send_north(picked):
        for c in picked:
            for other in norths:
                north_copy(c, other, n).start()
        for c in picked:
            u[rows(c, n), :] = wa[rows(c, n), :]

    split = sum(size for _, size in chunks[:early]) * north
    first.wait()
    for g in range(groups):
        loads[g].wait()
        along_x(g, 0, split)
    pl.semaphore_wait(barrier, north + deep - 2)
    send_north(range(early))
    if split < grid_x:
        for g in range(groups):
            along_x(g, split, grid_x - split)
        send_north(range(early, len(chunks)))

    pltpu.make_async_copy(symbols, symbols, table_sem.at[3]).wait()
    at_y, at_z = grid_x, grid_x + grid_y
    spot = lax.broadcasted_iota(jnp.int32, (part_y, grid_y), 0) + d * part_y
    along = lax.broadcasted_iota(jnp.int32, (part_y, grid_y), 1)
    column = jnp.sum(jnp.where(spot == along, symbols[:, at_y:at_z], 0.0), axis=1, keepdims=True)
    plane = column + symbols[:, at_z:]
    spot = lax.broadcasted_iota(jnp.int32, (share_x, grid_x), 0) + n * share_x
    along = lax.broadcasted_iota(jnp.int32, (share_x, grid_x), 1)
    column = jnp.sum(jnp.where(spot == along, symbols[:, :at_y], 0.0), axis=1, keepdims=True)
    for i in range(share_x):
        symbol = column[i : i + 1] + plane
        fac[pl.ds(i * part_y, part_y), :] = (1.0 - 0.2 * symbol) / (1.0 + 0.2 * symbol)

    mine = pl.ds(pl.multiple_of(d * part_y, part_y), part_y)
    tables[0].wait()
    for c in range(len(chunks)):
        north_landed(c)
        start, size = chunks[c]
        for i in range(0, size, 2):
            pair = min(2, size - i)
            lines = jnp.concatenate(
                [
                    jnp.concatenate(
                        [
                            u[pl.ds((start * north + s * size + i + k) * share_y, share_y), :]
                            for s in range(north)
                        ],
                        axis=0,
                    )
                    for k in range(pair)
                ],
                axis=1,
            )
            high, low = halves(lines)
            modes = jnp.dot(
                hy[...],
                jnp.concatenate([high, low, high], axis=0),
                preferred_element_type=jnp.float32,
            )
            for k in range(pair):
                v[start + i + k] = modes[:, k * lanes : (k + 1) * lanes]
        for other in deeps:
            deep_copy(c, other, d).start()
        r[d, pl.ds(start, size)] = v[pl.ds(start, size), mine]

    tables[1].wait()
    for c in range(len(chunks)):
        start, size = chunks[c]
        deep_landed(c)
        parts = [r[s, pl.ds(*chunks[c])].reshape(size * part_y, lanes) for s in range(deep)]
        factor = fac[pl.ds(start * part_y, size * part_y), :]
        for f in range(fields):
            lines = jnp.concatenate([p[:, f * share_z : (f + 1) * share_z] for p in parts], axis=1)
            high, low = halves(lines)
            modes = jnp.dot(
                jnp.concatenate([high, low, high], axis=1),
                hz[...],
                preferred_element_type=jnp.float32,
            )
            out[f, pl.ds(*chunks[c])] = (modes * factor).reshape(size, part_y, grid_z)

    sent = wa.at[pl.ds(0, (north - 1) * share_x * share_y)]
    pltpu.make_async_copy(sent, sent, ns_sem.at[0]).wait()
    sent = r.at[pl.ds(0, deep - 1)]
    pltpu.make_async_copy(sent, sent, ds_sem.at[0]).wait()


def local(north, deep, forcing, symbol_x, symbol_y, symbol_z):
    fields, grid_x, share_y, share_z = forcing.shape
    grid_y, grid_z = symbol_y.shape[0], symbol_z.shape[0]
    share_x, part_y = grid_x // north, grid_y // deep
    chunks = chunk_starts(share_x)
    lanes = fields * share_z

    modes = np.arange(grid_x).reshape(north, share_x)
    order = np.concatenate([modes[:, start : start + size].reshape(-1) for start, size in chunks])
    high, low = table_halves(transform_table(grid_x)[order])
    hx = np.concatenate([high, high, low], axis=1)
    high, low = table_halves(transform_table(grid_y))
    hy = np.concatenate([high, high, low], axis=1)
    high, low = table_halves(transform_table(grid_z))
    hz = np.concatenate([high, high, low], axis=0)

    groups = share_y // 4 if share_y % 4 == 0 else 1
    vmem = pl.BlockSpec(memory_space=pltpu.VMEM)
    buffers = [
        pltpu.VMEM((fields, share_y, share_z, grid_x), jnp.float32),
        pltpu.VMEM(hx.shape, jnp.bfloat16),
        pltpu.VMEM(hy.shape, jnp.bfloat16),
        pltpu.VMEM(hz.shape, jnp.bfloat16),
        pltpu.VMEM((grid_x * share_y, lanes), jnp.float32),
        pltpu.VMEM((grid_y * share_x, lanes), jnp.float32),
        pltpu.VMEM((share_x, grid_y, lanes), jnp.float32),
        pltpu.VMEM((deep, share_x, part_y, lanes), jnp.float32),
        pltpu.VMEM((share_x * part_y, grid_z), jnp.float32),
    ]
    result = fields * share_x * part_y * grid_z
    held = sum(math.prod(b.shape) * jnp.dtype(b.dtype).itemsize for b in buffers)
    return pl.pallas_call(
        functools.partial(kernel, (north, deep, chunks, min(EARLY, len(chunks)))),
        out_shape=pltpu.VMEM((fields, share_x, part_y, grid_z), jnp.float32),
        in_specs=[pl.BlockSpec(memory_space=pltpu.HBM)] * 7,
        out_specs=vmem,
        scratch_shapes=[
            pltpu.VMEM((1, grid_x + grid_y + grid_z), jnp.float32),
            *buffers,
            pltpu.SemaphoreType.DMA((groups,)),
            pltpu.SemaphoreType.DMA((4,)),
            pltpu.SemaphoreType.DMA((1,)),
            pltpu.SemaphoreType.DMA((len(chunks),)),
            pltpu.SemaphoreType.DMA((1,)),
            pltpu.SemaphoreType.DMA((len(chunks),)),
        ],
        compiler_params=pltpu.CompilerParams(
            collective_id=0, has_side_effects=True, vmem_limit_bytes=max(held + 2**23, 60 * 2**20 - 4 * result)
        ),
    )(
        forcing.transpose(0, 2, 3, 1),
        jnp.asarray(hx),
        jnp.asarray(hy),
        jnp.asarray(hz),
        symbol_x[None, :],
        symbol_y[None, :],
        symbol_z[None, :],
    )


def solution(mesh):
    placed = (P(None, None, "north", "deep"), P(), P(), P())
    return jax.shard_map(
        functools.partial(local, mesh.shape["north"], mesh.shape["deep"]),
        mesh=mesh,
        in_specs=placed,
        out_specs=P(None, "north", "deep", None),
        check_vma=False,
    )
```

```python
import functools
import math

import jax
import jax.numpy as jnp
import numpy as np
from jax import lax
from jax.experimental import pallas as pl
from jax.experimental.pallas import tpu as pltpu
from jax.sharding import PartitionSpec as P

CHUNKS = (1, 1, 2, 4, 4, 3, 1)
EARLY = 2
HELD = 3


def transform_table(count):
    rank = np.arange(count)
    odd = (2 * rank[:, None] + 1) * (2 * rank[None, :] + 1) % (8 * count)
    return (np.cos(np.pi / (4 * count) * odd) * np.sqrt(2.0 / count)).astype(np.float32)


def chunk_starts(share):
    unit = max(1, share // sum(CHUNKS))
    found, start = [], 0
    for weight in CHUNKS:
        size = min(unit * weight, share - start)
        if size > 0:
            found.append((start, size))
        start += size
    if start < share:
        found.append((start, share - start))
    return tuple(found)


def halves(values):
    high = values.astype(jnp.bfloat16)
    low = (values - high.astype(jnp.float32)).astype(jnp.bfloat16)
    return high, low


def table_halves(table):
    high = table.astype(jnp.bfloat16)
    low = (table - high.astype(np.float32)).astype(jnp.bfloat16)
    return high, low


def partners(me, count):
    found = []
    for step in range(count - 1, 0, -1):
        if count & (count - 1):
            found.append(lax.rem(me + step, count))
            continue
        other = me
        for bit in range(count.bit_length() - 1):
            if step >> bit & 1:
                other = other + (1 - 2 * ((me // 2**bit) % 2)) * 2**bit
        found.append(other)
    return found


def kernel(
    sizes, forcing, tx, ty, tz, gx, gy, gz, out, symbols, xin, hx, hy, hz, wa, u, v, r, fac,
    in_sem, table_sem, ns_sem, nr_sem, ds_sem, dr_sem,
):
    north, deep, chunks, early = sizes
    fields, share_y, share_z, grid_x = forcing.shape
    share_x, part_y = out.shape[1], out.shape[2]
    grid_y, grid_z = v.shape[1], out.shape[3]
    lanes = fields * share_z
    n, d = lax.axis_index("north"), lax.axis_index("deep")
    norths, deeps = partners(n, north), partners(d, deep)
    held = ()
    if deep == 4:
        far = jnp.where(d < 2, 3, 0)
        near, side = far + 1 - 2 * (far % 2), d + 1 - 2 * (d % 2)
        deeps, held = (far, side), (near,)

    barrier = pltpu.get_barrier_semaphore()
    for other in (*deeps, *held):
        pl.semaphore_signal(barrier, device_id={"deep": other}, device_id_type=pl.DeviceIdType.MESH)
    for other in norths:
        pl.semaphore_signal(barrier, device_id={"north": other}, device_id_type=pl.DeviceIdType.MESH)

    first = pltpu.make_async_copy(tx, hx, table_sem.at[0])
    first.start()
    groups = in_sem.shape[0]
    per = share_y // groups
    loads = []
    for g in range(groups):
        part = (slice(None), pl.ds(g * per, per))
        loads.append(pltpu.make_async_copy(forcing.at[part], xin.at[part], in_sem.at[g]))
        loads[-1].start()
    tables = [pltpu.make_async_copy(source, target, table_sem.at[k + 1]) for k, (source, target) in enumerate(((ty, hy), (tz, hz)))]
    for table in tables:
        table.start()
    at = 0
    for source in (gx, gy, gz):
        span = pl.ds(at, source.shape[1])
        pltpu.make_async_copy(source, symbols.at[:, span], table_sem.at[3]).start()
        at += source.shape[1]

    pair = 2 if per % 2 == 0 else 1

    def along_x(g, start, count):
        for y in range(g * per, (g + 1) * per, pair):
            high, low = halves(
                jnp.concatenate([xin[f, y + k] for k in range(pair) for f in range(fields)], axis=0)
            )
            modes = lax.dot_general(
                hx[pl.ds(start, count), :],
                jnp.concatenate([high, low, high], axis=1),
                (((1,), (1,)), ((), ())),
                preferred_element_type=jnp.float32,
            )
            for k in range(pair):
                wa[pl.ds(start * share_y + y + k, count, stride=share_y), :] = modes[
                    :, k * lanes : (k + 1) * lanes
                ]

    def rows(c, other):
        start, size = chunks[c]
        at = (start * north + other * size) * share_y
        return pl.ds(pl.multiple_of(at, share_y), size * share_y)

    def north_copy(c, target, source):
        return pltpu.make_async_remote_copy(
            src_ref=wa.at[rows(c, target)],
            dst_ref=u.at[rows(c, source)],
            send_sem=ns_sem.at[0],
            recv_sem=nr_sem.at[c],
            device_id={"north": target},
            device_id_type=pl.DeviceIdType.MESH,
        )

    def north_landed(c):
        every = u.at[pl.ds(0, (north - 1) * chunks[c][1] * share_y)]
        pltpu.make_async_copy(every, every, nr_sem.at[c]).wait()

    def deep_copy(c, target, source):
        return pltpu.make_async_remote_copy(
            src_ref=v.at[pl.ds(*chunks[c]), pl.ds(pl.multiple_of(target * part_y, part_y), part_y)],
            dst_ref=r.at[source, pl.ds(*chunks[c])],
            send_sem=ds_sem.at[0],
            recv_sem=dr_sem.at[c],
            device_id={"deep": target},
            device_id_type=pl.DeviceIdType.MESH,
        )

    def deep_landed(c):
        every = r.at[pl.ds(0, deep - 1), pl.ds(0, chunks[c][1])]
        pltpu.make_async_copy(every, every, dr_sem.at[c]).wait()

    def send_north(picked):
        for c in picked:
            for other in norths:
                north_copy(c, other, n).start()
        for c in picked:
            u[rows(c, n), :] = wa[rows(c, n), :]

    split = sum(size for _, size in chunks[:early]) * north
    first.wait()
    for g in range(groups):
        loads[g].wait()
        along_x(g, 0, split)
    pl.semaphore_wait(barrier, north + deep - 2)
    send_north(range(early))
    if split < grid_x:
        for g in range(groups):
            along_x(g, split, grid_x - split)
        send_north(range(early, len(chunks)))

    pltpu.make_async_copy(symbols, symbols, table_sem.at[3]).wait()
    at_y, at_z = grid_x, grid_x + grid_y
    spot = lax.broadcasted_iota(jnp.int32, (part_y, grid_y), 0) + d * part_y
    along = lax.broadcasted_iota(jnp.int32, (part_y, grid_y), 1)
    column = jnp.sum(jnp.where(spot == along, symbols[:, at_y:at_z], 0.0), axis=1, keepdims=True)
    plane = column + symbols[:, at_z:]
    spot = lax.broadcasted_iota(jnp.int32, (share_x, grid_x), 0) + n * share_x
    along = lax.broadcasted_iota(jnp.int32, (share_x, grid_x), 1)
    column = jnp.sum(jnp.where(spot == along, symbols[:, :at_y], 0.0), axis=1, keepdims=True)
    for i in range(share_x):
        symbol = column[i : i + 1] + plane
        fac[pl.ds(i * part_y, part_y), :] = (1.0 - 0.2 * symbol) / (1.0 + 0.2 * symbol)

    free = max(0, len(chunks) - HELD)
    mine = pl.ds(pl.multiple_of(d * part_y, part_y), part_y)
    tables[0].wait()
    for c in range(len(chunks)):
        north_landed(c)
        start, size = chunks[c]
        for i in range(0, size, 2):
            pair = min(2, size - i)
            lines = jnp.concatenate(
                [
                    jnp.concatenate(
                        [
                            u[pl.ds((start * north + s * size + i + k) * share_y, share_y), :]
                            for s in range(north)
                        ],
                        axis=0,
                    )
                    for k in range(pair)
                ],
                axis=1,
            )
            high, low = halves(lines)
            modes = jnp.dot(
                hy[...],
                jnp.concatenate([high, low, high], axis=0),
                preferred_element_type=jnp.float32,
            )
            for k in range(pair):
                v[start + i + k] = modes[:, k * lanes : (k + 1) * lanes]
        last = c == len(chunks) - 1
        for other in deeps if c >= free else (*deeps[:1], *held, *deeps[1:]):
            deep_copy(c, other, d).start()
        for late in range(free, len(chunks)) if last else ():
            for other in held:
                deep_copy(late, other, d).start()
        r[d, pl.ds(start, size)] = v[pl.ds(start, size), mine]

    tables[1].wait()
    for c in range(len(chunks)):
        start, size = chunks[c]
        deep_landed(c)
        parts = [r[s, pl.ds(*chunks[c])].reshape(size * part_y, lanes) for s in range(deep)]
        factor = fac[pl.ds(start * part_y, size * part_y), :]
        for f in range(fields):
            lines = jnp.concatenate([p[:, f * share_z : (f + 1) * share_z] for p in parts], axis=1)
            high, low = halves(lines)
            modes = jnp.dot(
                jnp.concatenate([high, low, high], axis=1),
                hz[...],
                preferred_element_type=jnp.float32,
            )
            out[f, pl.ds(*chunks[c])] = (modes * factor).reshape(size, part_y, grid_z)

    sent = wa.at[pl.ds(0, (north - 1) * share_x * share_y)]
    pltpu.make_async_copy(sent, sent, ns_sem.at[0]).wait()
    sent = r.at[pl.ds(0, deep - 1)]
    pltpu.make_async_copy(sent, sent, ds_sem.at[0]).wait()


def local(north, deep, forcing, symbol_x, symbol_y, symbol_z):
    fields, grid_x, share_y, share_z = forcing.shape
    grid_y, grid_z = symbol_y.shape[0], symbol_z.shape[0]
    share_x, part_y = grid_x // north, grid_y // deep
    chunks = chunk_starts(share_x)
    lanes = fields * share_z

    modes = np.arange(grid_x).reshape(north, share_x)
    order = np.concatenate([modes[:, start : start + size].reshape(-1) for start, size in chunks])
    high, low = table_halves(transform_table(grid_x)[order])
    hx = np.concatenate([high, high, low], axis=1)
    high, low = table_halves(transform_table(grid_y))
    hy = np.concatenate([high, high, low], axis=1)
    high, low = table_halves(transform_table(grid_z))
    hz = np.concatenate([high, high, low], axis=0)

    groups = share_y // 4 if share_y % 4 == 0 else 1
    vmem = pl.BlockSpec(memory_space=pltpu.VMEM)
    buffers = [
        pltpu.VMEM((fields, share_y, share_z, grid_x), jnp.float32),
        pltpu.VMEM(hx.shape, jnp.bfloat16),
        pltpu.VMEM(hy.shape, jnp.bfloat16),
        pltpu.VMEM(hz.shape, jnp.bfloat16),
        pltpu.VMEM((grid_x * share_y, lanes), jnp.float32),
        pltpu.VMEM((grid_y * share_x, lanes), jnp.float32),
        pltpu.VMEM((share_x, grid_y, lanes), jnp.float32),
        pltpu.VMEM((deep, share_x, part_y, lanes), jnp.float32),
        pltpu.VMEM((share_x * part_y, grid_z), jnp.float32),
    ]
    result = fields * share_x * part_y * grid_z
    held = sum(math.prod(b.shape) * jnp.dtype(b.dtype).itemsize for b in buffers)
    return pl.pallas_call(
        functools.partial(kernel, (north, deep, chunks, min(EARLY, len(chunks)))),
        out_shape=pltpu.VMEM((fields, share_x, part_y, grid_z), jnp.float32),
        in_specs=[pl.BlockSpec(memory_space=pltpu.HBM)] * 7,
        out_specs=vmem,
        scratch_shapes=[
            pltpu.VMEM((1, grid_x + grid_y + grid_z), jnp.float32),
            *buffers,
            pltpu.SemaphoreType.DMA((groups,)),
            pltpu.SemaphoreType.DMA((4,)),
            pltpu.SemaphoreType.DMA((1,)),
            pltpu.SemaphoreType.DMA((len(chunks),)),
            pltpu.SemaphoreType.DMA((1,)),
            pltpu.SemaphoreType.DMA((len(chunks),)),
        ],
        compiler_params=pltpu.CompilerParams(
            collective_id=0, has_side_effects=True, vmem_limit_bytes=max(held + 2**23, 60 * 2**20 - 4 * result)
        ),
    )(
        forcing.transpose(0, 2, 3, 1),
        jnp.asarray(hx),
        jnp.asarray(hy),
        jnp.asarray(hz),
        symbol_x[None, :],
        symbol_y[None, :],
        symbol_z[None, :],
    )


def solution(mesh):
    placed = (P(None, None, "north", "deep"), P(), P(), P())
    return jax.shard_map(
        functools.partial(local, mesh.shape["north"], mesh.shape["deep"]),
        mesh=mesh,
        in_specs=placed,
        out_specs=P(None, "north", "deep", None),
        check_vma=False,
    )
```

```python
import functools
import math

import jax
import jax.numpy as jnp
import numpy as np
from jax import lax
from jax.experimental import pallas as pl
from jax.experimental.pallas import tpu as pltpu
from jax.sharding import PartitionSpec as P

CHUNKS = (1, 2, 1, 4, 4, 3, 1)
EARLY = 2
HELD = 3
AHEAD = 1
RELAY = 3


def transform_table(count):
    rank = np.arange(count)
    odd = (2 * rank[:, None] + 1) * (2 * rank[None, :] + 1) % (8 * count)
    return (np.cos(np.pi / (4 * count) * odd) * np.sqrt(2.0 / count)).astype(np.float32)


def chunk_starts(share):
    unit = max(1, share // sum(CHUNKS))
    found, start = [], 0
    for weight in CHUNKS:
        size = min(unit * weight, share - start)
        if size > 0:
            found.append((start, size))
        start += size
    if start < share:
        found.append((start, share - start))
    return tuple(found)


def halves(values):
    high = values.astype(jnp.bfloat16)
    low = (values - high.astype(jnp.float32)).astype(jnp.bfloat16)
    return high, low


def table_halves(table):
    high = table.astype(jnp.bfloat16)
    low = (table - high.astype(np.float32)).astype(jnp.bfloat16)
    return high, low


def partners(me, count):
    found = []
    for step in range(count - 1, 0, -1):
        if count & (count - 1):
            found.append(lax.rem(me + step, count))
            continue
        other = me
        for bit in range(count.bit_length() - 1):
            if step >> bit & 1:
                other = other + (1 - 2 * ((me // 2**bit) % 2)) * 2**bit
        found.append(other)
    return found


def kernel(
    sizes, forcing, tx, ty, tz, gx, gy, gz, out, symbols, xin, hx, hy, hz, wa, u, v, r, fac, ein, eu, ev,
    in_sem, table_sem, ns_sem, nr_sem, ds_sem, dr_sem, round_sem, ahead_sem,
):
    north, deep, chunks, early = sizes
    fields, share_y, share_z, grid_x = forcing.shape
    share_x, part_y = out.shape[1], out.shape[2]
    grid_y, grid_z = v.shape[1], out.shape[3]
    lanes, rounds = fields * share_z, max(0, deep - 2)
    ahead = deep == 4 and len(chunks) > RELAY
    n, d = lax.axis_index("north"), lax.axis_index("deep")
    norths, deeps = partners(n, north), partners(d, deep)
    held = ()
    if deep == 4:
        far = jnp.where(d < 2, 3, 0)
        near, side = far + 1 - 2 * (far % 2), d + 1 - 2 * (d % 2)
        deeps, held = (far, side), (near,)

    barrier = pltpu.get_barrier_semaphore()
    inner = (d > 0).astype(jnp.int32) + (d < deep - 1).astype(jnp.int32)

    def signal_beside(semaphore):
        for other, there in ((d - 1, d > 0), (d + 1, d < deep - 1)):
            @pl.when(there)
            def _():
                pl.semaphore_signal(
                    semaphore, device_id={"deep": other}, device_id_type=pl.DeviceIdType.MESH
                )

    signal_beside(barrier)
    for other in norths:
        pl.semaphore_signal(barrier, device_id={"north": other}, device_id_type=pl.DeviceIdType.MESH)

    first = pltpu.make_async_copy(tx, hx, table_sem.at[0])
    first.start()
    groups = in_sem.shape[0]
    per = share_y // groups
    loads = []
    for g in range(groups):
        part = (slice(None), pl.ds(g * per, per))
        loads.append(pltpu.make_async_copy(forcing.at[part], xin.at[part], in_sem.at[g]))
        loads[-1].start()
    tables = [pltpu.make_async_copy(source, target, table_sem.at[k + 1]) for k, (source, target) in enumerate(((ty, hy), (tz, hz)))]
    pair = 2 if per % 2 == 0 else 1

    def along_x(g, start, count):
        for y in range(g * per, (g + 1) * per, pair):
            high, low = halves(
                jnp.concatenate([xin[f, y + k] for k in range(pair) for f in range(fields)], axis=0)
            )
            both = lax.dot_general(
                hx[pl.ds(2 * start, 2 * count), :],
                jnp.concatenate([high, low], axis=1),
                (((1,), (1,)), ((), ())),
                preferred_element_type=jnp.float32,
            )
            modes = both[:count] + both[count:]
            for k in range(pair):
                wa[pl.ds(start * share_y + y + k, count, stride=share_y), :] = modes[
                    :, k * lanes : (k + 1) * lanes
                ]

    def rows(c, other):
        start, size = chunks[c]
        at = (start * north + other * size) * share_y
        return pl.ds(pl.multiple_of(at, share_y), size * share_y)

    def north_copy(c, target, source):
        return pltpu.make_async_remote_copy(
            src_ref=wa.at[rows(c, target)],
            dst_ref=u.at[rows(c, source)],
            send_sem=ns_sem.at[0],
            recv_sem=nr_sem.at[c],
            device_id={"north": target},
            device_id_type=pl.DeviceIdType.MESH,
        )

    def north_landed(c):
        every = u.at[pl.ds(0, (north - 1) * chunks[c][1] * share_y)]
        pltpu.make_async_copy(every, every, nr_sem.at[c]).wait()

    def deep_copy(c, target, source):
        return pltpu.make_async_remote_copy(
            src_ref=v.at[pl.ds(*chunks[c]), pl.ds(pl.multiple_of(target * part_y, part_y), part_y)],
            dst_ref=r.at[source, pl.ds(*chunks[c])],
            send_sem=ds_sem.at[0],
            recv_sem=dr_sem.at[c],
            device_id={"deep": target},
            device_id_type=pl.DeviceIdType.MESH,
        )

    def deep_landed(c):
        def take(count):
            every = r.at[pl.ds(0, count), pl.ds(0, chunks[c][1])]
            pltpu.make_async_copy(every, every, dr_sem.at[c]).wait()

        if ahead and c == AHEAD:
            pl.when(d == 1)(lambda: take(deep - 2))
            pl.when(d != 1)(lambda: take(deep - 1))
        else:
            take(deep - 1)

    def ahead_rows(other, count=1):
        size = chunks[AHEAD][1] * share_y
        return pl.ds(pl.multiple_of(other * size, size), count * size)

    def ahead_down():
        start, size = chunks[AHEAD]
        return pltpu.make_async_remote_copy(
            src_ref=wa.at[pl.ds(start * north * share_y, size * north * share_y)],
            dst_ref=ein,
            send_sem=ahead_sem.at[0],
            recv_sem=ahead_sem.at[1],
            device_id={"deep": 1},
            device_id_type=pl.DeviceIdType.MESH,
        )

    def ahead_across(target, source):
        return pltpu.make_async_remote_copy(
            src_ref=ein.at[ahead_rows(target)],
            dst_ref=eu.at[ahead_rows(source)],
            send_sem=ahead_sem.at[2],
            recv_sem=ahead_sem.at[3],
            device_id={"north": target},
            device_id_type=pl.DeviceIdType.MESH,
        )

    def ahead_on():
        return pltpu.make_async_remote_copy(
            src_ref=ev.at[:, pl.ds(0, part_y)],
            dst_ref=r.at[2, pl.ds(*chunks[AHEAD])],
            send_sem=ahead_sem.at[4],
            recv_sem=dr_sem.at[AHEAD],
            device_id={"deep": 0},
            device_id_type=pl.DeviceIdType.MESH,
        )

    def send_north(picked):
        for c in picked:
            for other in norths:
                north_copy(c, other, n).start()
        for c in picked:
            u[rows(c, n), :] = wa[rows(c, n), :]

    split = sum(size for _, size in chunks[:early]) * north
    first.wait()
    for g in range(groups):
        loads[g].wait()
    for g in range(groups):
        along_x(g, 0, split)
    for table in tables:
        table.start()
    at = 0
    for source in (gx, gy, gz):
        span = pl.ds(at, source.shape[1])
        pltpu.make_async_copy(source, symbols.at[:, span], table_sem.at[3]).start()
        at += source.shape[1]
    pl.semaphore_wait(barrier, north - 1 + inner)
    if ahead:
        pl.when(d == 2)(lambda: ahead_down().start())
    send_north(range(early))
    if rounds:
        signal_beside(round_sem.at[0])
    if split < grid_x:
        for g in range(groups):
            along_x(g, split, grid_x - split)
        send_north(range(early, len(chunks)))

    for k in range(rounds - 1):
        pl.semaphore_wait(round_sem.at[k], inner)
        signal_beside(round_sem.at[k + 1])
    pltpu.make_async_copy(symbols, symbols, table_sem.at[3]).wait()
    at_y, at_z = grid_x, grid_x + grid_y
    spot = lax.broadcasted_iota(jnp.int32, (part_y, grid_y), 0) + d * part_y
    along = lax.broadcasted_iota(jnp.int32, (part_y, grid_y), 1)
    column = jnp.sum(jnp.where(spot == along, symbols[:, at_y:at_z], 0.0), axis=1, keepdims=True)
    plane = column + symbols[:, at_z:]
    spot = lax.broadcasted_iota(jnp.int32, (share_x, grid_x), 0) + n * share_x
    along = lax.broadcasted_iota(jnp.int32, (share_x, grid_x), 1)
    column = jnp.sum(jnp.where(spot == along, symbols[:, :at_y], 0.0), axis=1, keepdims=True)
    for i in range(share_x):
        symbol = column[i : i + 1] + plane
        fac[pl.ds(i * part_y, part_y), :] = (1.0 - 0.2 * symbol) / (1.0 + 0.2 * symbol)

    def along_y(blocks, base, size, i, pair, count):
        lines = jnp.concatenate(
            [
                jnp.concatenate(
                    [blocks[pl.ds(base + (s * size + i + k) * share_y, share_y), :] for s in range(north)],
                    axis=0,
                )
                for k in range(pair)
            ],
            axis=1,
        )
        high, low = halves(lines)
        return jnp.dot(
            hy[pl.ds(0, count), :],
            jnp.concatenate([high, low, high], axis=0),
            preferred_element_type=jnp.float32,
        )

    free = max(0, len(chunks) - HELD)
    mine = pl.ds(pl.multiple_of(d * part_y, part_y), part_y)
    tables[0].wait()
    for c in range(len(chunks)):
        north_landed(c)
        if c == 0 and rounds:
            pl.semaphore_wait(round_sem.at[rounds - 1], inner)
        start, size = chunks[c]
        for i in range(0, size, 2):
            pair = min(2, size - i)
            modes = along_y(u, start * north * share_y, size, i, pair, grid_y)
            for k in range(pair):
                v[start + i + k] = modes[:, k * lanes : (k + 1) * lanes]
        last = c == len(chunks) - 1
        if ahead and c == AHEAD:
            @pl.when(d != 2)
            def _():
                for other in (deeps[0], *held):
                    deep_copy(c, other, d).start()

            deep_copy(c, deeps[1], d).start()
        else:
            for other in deeps if c >= free else (*deeps[:1], *held, *deeps[1:]):
                deep_copy(c, other, d).start()
        for late in range(free, len(chunks)) if last else ():
            for other in held:
                deep_copy(late, other, d).start()
        r[d, pl.ds(start, size)] = v[pl.ds(start, size), mine]
        if ahead and c == RELAY:
            @pl.when(d == 1)
            def _():
                ahead_down().wait_recv()
                for other in norths:
                    ahead_across(other, n).start()
                eu[ahead_rows(n), :] = ein[ahead_rows(n), :]

    if ahead:
        @pl.when(d == 1)
        def _():
            start, size = chunks[AHEAD]
            every = eu.at[ahead_rows(0, north - 1)]
            pltpu.make_async_copy(every, every, ahead_sem.at[3]).wait()
            for i in range(0, size, 2):
                pair = min(2, size - i)
                modes = along_y(eu, 0, size, i, pair, 2 * part_y)
                for k in range(pair):
                    ev[i + k] = modes[:, k * lanes : (k + 1) * lanes]
            ahead_on().start()
            r[2, pl.ds(start, size)] = ev[:, part_y:]

    tables[1].wait()
    for c in range(len(chunks)):
        start, size = chunks[c]
        deep_landed(c)
        parts = [r[s, pl.ds(*chunks[c])].reshape(size * part_y, lanes) for s in range(deep)]
        factor = fac[pl.ds(start * part_y, size * part_y), :]
        for f in range(fields):
            lines = jnp.concatenate([p[:, f * share_z : (f + 1) * share_z] for p in parts], axis=1)
            high, low = halves(lines)
            modes = jnp.dot(
                jnp.concatenate([high, low, high], axis=1),
                hz[...],
                preferred_element_type=jnp.float32,
            )
            out[f, pl.ds(*chunks[c])] = (modes * factor).reshape(size, part_y, grid_z)

    sent = wa.at[pl.ds(0, (north - 1) * share_x * share_y)]
    pltpu.make_async_copy(sent, sent, ns_sem.at[0]).wait()
    every = r.at[pl.ds(0, deep - 1)]
    if ahead:
        @pl.when(d == 2)
        def _():
            rest = share_x * (deep - 1) - 2 * chunks[AHEAD][1]
            some = wa.at[pl.ds(0, rest * part_y)]
            pltpu.make_async_copy(some, some, ds_sem.at[0]).wait()
            ahead_down().wait_send()

        @pl.when(d != 2)
        def _():
            pltpu.make_async_copy(every, every, ds_sem.at[0]).wait()

        @pl.when(d == 1)
        def _():
            sent = ein.at[ahead_rows(0, north - 1)]
            pltpu.make_async_copy(sent, sent, ahead_sem.at[2]).wait()
            ahead_on().wait_send()
    else:
        pltpu.make_async_copy(every, every, ds_sem.at[0]).wait()


def local(north, deep, forcing, symbol_x, symbol_y, symbol_z):
    fields, grid_x, share_y, share_z = forcing.shape
    grid_y, grid_z = symbol_y.shape[0], symbol_z.shape[0]
    share_x, part_y = grid_x // north, grid_y // deep
    chunks = chunk_starts(share_x)
    lanes = fields * share_z

    modes = np.arange(grid_x).reshape(north, share_x)
    order = np.concatenate([modes[:, start : start + size].reshape(-1) for start, size in chunks])
    high, low = table_halves(transform_table(grid_x)[order])
    split = sum(size for _, size in chunks[:EARLY]) * north
    hx = np.concatenate(
        [
            np.block([[high[part], high[part]], [low[part], np.zeros_like(low[part])]])
            for part in (slice(0, split), slice(split, grid_x))
        ],
        axis=0,
    )
    high, low = table_halves(transform_table(grid_y))
    hy = np.concatenate([high, high, low], axis=1)
    high, low = table_halves(transform_table(grid_z))
    hz = np.concatenate([high, high, low], axis=0)

    groups, extra = 1, chunks[min(AHEAD, len(chunks) - 1)][1]
    vmem = pl.BlockSpec(memory_space=pltpu.VMEM)
    buffers = [
        pltpu.VMEM((fields, share_y, share_z, grid_x), jnp.float32),
        pltpu.VMEM(hx.shape, jnp.bfloat16),
        pltpu.VMEM(hy.shape, jnp.bfloat16),
        pltpu.VMEM(hz.shape, jnp.bfloat16),
        pltpu.VMEM((grid_x * share_y, lanes), jnp.float32),
        pltpu.VMEM((grid_y * share_x, lanes), jnp.float32),
        pltpu.VMEM((share_x, grid_y, lanes), jnp.float32),
        pltpu.VMEM((deep, share_x, part_y, lanes), jnp.float32),
        pltpu.VMEM((share_x * part_y, grid_z), jnp.float32),
        pltpu.VMEM((extra * north * share_y, lanes), jnp.float32),
        pltpu.VMEM((extra * north * share_y, lanes), jnp.float32),
        pltpu.VMEM((extra, 2 * part_y, lanes), jnp.float32),
    ]
    result = fields * share_x * part_y * grid_z
    held = sum(math.prod(b.shape) * jnp.dtype(b.dtype).itemsize for b in buffers)
    return pl.pallas_call(
        functools.partial(kernel, (north, deep, chunks, min(EARLY, len(chunks)))),
        out_shape=pltpu.VMEM((fields, share_x, part_y, grid_z), jnp.float32),
        in_specs=[pl.BlockSpec(memory_space=pltpu.HBM)] * 7,
        out_specs=vmem,
        scratch_shapes=[
            pltpu.VMEM((1, grid_x + grid_y + grid_z), jnp.float32),
            *buffers,
            pltpu.SemaphoreType.DMA((groups,)),
            pltpu.SemaphoreType.DMA((4,)),
            pltpu.SemaphoreType.DMA((1,)),
            pltpu.SemaphoreType.DMA((len(chunks),)),
            pltpu.SemaphoreType.DMA((1,)),
            pltpu.SemaphoreType.DMA((len(chunks),)),
            pltpu.SemaphoreType.REGULAR((max(1, deep - 2),)),
            pltpu.SemaphoreType.DMA((5,)),
        ],
        compiler_params=pltpu.CompilerParams(
            collective_id=0, has_side_effects=True, vmem_limit_bytes=max(held + 2**23, 60 * 2**20 - 4 * result)
        ),
    )(
        forcing.transpose(0, 2, 3, 1),
        jnp.asarray(hx),
        jnp.asarray(hy),
        jnp.asarray(hz),
        symbol_x[None, :],
        symbol_y[None, :],
        symbol_z[None, :],
    )


def solution(mesh):
    placed = (P(None, None, "north", "deep"), P(), P(), P())
    return jax.shard_map(
        functools.partial(local, mesh.shape["north"], mesh.shape["deep"]),
        mesh=mesh,
        in_specs=placed,
        out_specs=P(None, "north", "deep", None),
        check_vma=False,
    )
```

```python
import functools
import math

import jax
import jax.numpy as jnp
import numpy as np
from jax import lax
from jax.experimental import pallas as pl
from jax.experimental.pallas import tpu as pltpu
from jax.sharding import PartitionSpec as P

CHUNKS = (1, 2, 1, 4, 4, 3, 1)
EARLY = 2
HELD = 3
AHEAD = 1
RELAY = 3
NEAR_NOW = (0, 1, 2, 3)
NEAR_AFTER = {}
NEAR_THEN = {3: (4, 5, 6)}


def transform_table(count):
    rank = np.arange(count)
    odd = (2 * rank[:, None] + 1) * (2 * rank[None, :] + 1) % (8 * count)
    return (np.cos(np.pi / (4 * count) * odd) * np.sqrt(2.0 / count)).astype(np.float32)


def chunk_starts(share):
    unit = max(1, share // sum(CHUNKS))
    found, start = [], 0
    for weight in CHUNKS:
        size = min(unit * weight, share - start)
        if size > 0:
            found.append((start, size))
        start += size
    if start < share:
        found.append((start, share - start))
    return tuple(found)


def halves(values):
    high = values.astype(jnp.bfloat16)
    low = (values - high.astype(jnp.float32)).astype(jnp.bfloat16)
    return high, low


def table_halves(table):
    high = table.astype(jnp.bfloat16)
    low = (table - high.astype(np.float32)).astype(jnp.bfloat16)
    return high, low


def partners(me, count):
    found = []
    for step in range(count - 1, 0, -1):
        if count & (count - 1):
            found.append(lax.rem(me + step, count))
            continue
        other = me
        for bit in range(count.bit_length() - 1):
            if step >> bit & 1:
                other = other + (1 - 2 * ((me // 2**bit) % 2)) * 2**bit
        found.append(other)
    return found


def kernel(
    sizes, forcing, tx, ty, tz, gx, gy, gz, out, symbols, xin, hx, hy, hz, wa, u, v, r, fac, ein, eu, ev,
    in_sem, table_sem, ns_sem, nr_sem, ds_sem, dr_sem, round_sem, ahead_sem,
):
    north, deep, chunks, early = sizes
    fields, share_y, share_z, grid_x = forcing.shape
    share_x, part_y = out.shape[1], out.shape[2]
    grid_y, grid_z = v.shape[1], out.shape[3]
    lanes, rounds = fields * share_z, max(0, deep - 2)
    ahead = deep == 4 and len(chunks) > RELAY
    n, d = lax.axis_index("north"), lax.axis_index("deep")
    norths, deeps = partners(n, north), partners(d, deep)
    held, inward = (), (d == 1) | (d == 2)
    if deep == 4:
        far = jnp.where(d < 2, 3, 0)
        near, side = far + 1 - 2 * (far % 2), d + 1 - 2 * (d % 2)
        deeps, held = (far, side), (near,)

    first = pltpu.make_async_copy(tx, hx, table_sem.at[0])
    groups = in_sem.shape[0]
    per = share_y // groups
    loads = []
    for g in range(groups):
        part = (slice(None), pl.ds(g * per, per))
        loads.append(pltpu.make_async_copy(forcing.at[part], xin.at[part], in_sem.at[g]))
        loads[-1].start()
    first.start()

    barrier = pltpu.get_barrier_semaphore()
    inner = (d > 0).astype(jnp.int32) + (d < deep - 1).astype(jnp.int32)

    def signal_beside(semaphore):
        for other, there in ((d - 1, d > 0), (d + 1, d < deep - 1)):
            @pl.when(there)
            def _():
                pl.semaphore_signal(
                    semaphore, device_id={"deep": other}, device_id_type=pl.DeviceIdType.MESH
                )

    signal_beside(barrier)
    for other in norths:
        pl.semaphore_signal(barrier, device_id={"north": other}, device_id_type=pl.DeviceIdType.MESH)
    tables = [pltpu.make_async_copy(source, target, table_sem.at[k + 1]) for k, (source, target) in enumerate(((ty, hy), (tz, hz)))]
    pair = 2 if per % 2 == 0 else 1

    def along_x(g, start, count):
        for y in range(g * per, (g + 1) * per, pair):
            high, low = halves(
                jnp.concatenate([xin[f, y + k] for k in range(pair) for f in range(fields)], axis=0)
            )
            both = lax.dot_general(
                hx[pl.ds(2 * start, 2 * count), :],
                jnp.concatenate([high, low], axis=1),
                (((1,), (1,)), ((), ())),
                preferred_element_type=jnp.float32,
            )
            modes = both[:count] + both[count:]
            for k in range(pair):
                wa[pl.ds(start * share_y + y + k, count, stride=share_y), :] = modes[
                    :, k * lanes : (k + 1) * lanes
                ]

    def rows(c, other):
        start, size = chunks[c]
        at = (start * north + other * size) * share_y
        return pl.ds(pl.multiple_of(at, share_y), size * share_y)

    def north_copy(c, target, source):
        return pltpu.make_async_remote_copy(
            src_ref=wa.at[rows(c, target)],
            dst_ref=u.at[rows(c, source)],
            send_sem=ns_sem.at[0],
            recv_sem=nr_sem.at[c],
            device_id={"north": target},
            device_id_type=pl.DeviceIdType.MESH,
        )

    def north_landed(c):
        every = u.at[pl.ds(0, (north - 1) * chunks[c][1] * share_y)]
        pltpu.make_async_copy(every, every, nr_sem.at[c]).wait()

    def deep_copy(c, target, source):
        return pltpu.make_async_remote_copy(
            src_ref=v.at[pl.ds(*chunks[c]), pl.ds(pl.multiple_of(target * part_y, part_y), part_y)],
            dst_ref=r.at[source, pl.ds(*chunks[c])],
            send_sem=ds_sem.at[0],
            recv_sem=dr_sem.at[c],
            device_id={"deep": target},
            device_id_type=pl.DeviceIdType.MESH,
        )

    def deep_landed(c):
        def take(count):
            every = r.at[pl.ds(0, count), pl.ds(0, chunks[c][1])]
            pltpu.make_async_copy(every, every, dr_sem.at[c]).wait()

        if ahead and c == AHEAD:
            pl.when(d == 1)(lambda: take(deep - 2))
            pl.when(d != 1)(lambda: take(deep - 1))
        else:
            take(deep - 1)

    def ahead_rows(other, count=1):
        size = chunks[AHEAD][1] * share_y
        return pl.ds(pl.multiple_of(other * size, size), count * size)

    def ahead_down():
        start, size = chunks[AHEAD]
        return pltpu.make_async_remote_copy(
            src_ref=wa.at[pl.ds(start * north * share_y, size * north * share_y)],
            dst_ref=ein,
            send_sem=ahead_sem.at[2],
            recv_sem=ahead_sem.at[0],
            device_id={"deep": 1},
            device_id_type=pl.DeviceIdType.MESH,
        )

    def ahead_across(target, source):
        return pltpu.make_async_remote_copy(
            src_ref=ein.at[ahead_rows(target)],
            dst_ref=eu.at[ahead_rows(source)],
            send_sem=ahead_sem.at[2],
            recv_sem=ahead_sem.at[1],
            device_id={"north": target},
            device_id_type=pl.DeviceIdType.MESH,
        )

    def ahead_on():
        return pltpu.make_async_remote_copy(
            src_ref=ev.at[:, pl.ds(0, part_y)],
            dst_ref=r.at[2, pl.ds(*chunks[AHEAD])],
            send_sem=ds_sem.at[0],
            recv_sem=dr_sem.at[AHEAD],
            device_id={"deep": 0},
            device_id_type=pl.DeviceIdType.MESH,
        )

    def send_north(picked):
        for c in picked:
            for other in norths:
                north_copy(c, other, n).start()
        for c in picked:
            u[rows(c, n), :] = wa[rows(c, n), :]

    split = sum(size for _, size in chunks[:early]) * north
    first.wait()
    for g in range(groups):
        loads[g].wait()
    for g in range(groups):
        along_x(g, 0, split)
    for table in tables:
        table.start()
    at = 0
    for source in (gx, gy, gz):
        span = pl.ds(at, source.shape[1])
        pltpu.make_async_copy(source, symbols.at[:, span], table_sem.at[3]).start()
        at += source.shape[1]
    pl.semaphore_wait(barrier, north - 1 + inner)
    if ahead:
        pl.when(d == 2)(lambda: ahead_down().start())
    send_north(range(early))
    if rounds:
        signal_beside(round_sem.at[0])
    if split < grid_x:
        for g in range(groups):
            along_x(g, split, grid_x - split)
        send_north(range(early, len(chunks)))

    for k in range(rounds - 1):
        pl.semaphore_wait(round_sem.at[k], inner)
        signal_beside(round_sem.at[k + 1])
    pltpu.make_async_copy(symbols, symbols, table_sem.at[3]).wait()
    at_y, at_z = grid_x, grid_x + grid_y
    spot = lax.broadcasted_iota(jnp.int32, (part_y, grid_y), 0) + d * part_y
    along = lax.broadcasted_iota(jnp.int32, (part_y, grid_y), 1)
    column = jnp.sum(jnp.where(spot == along, symbols[:, at_y:at_z], 0.0), axis=1, keepdims=True)
    plane = column + symbols[:, at_z:]
    spot = lax.broadcasted_iota(jnp.int32, (share_x, grid_x), 0) + n * share_x
    along = lax.broadcasted_iota(jnp.int32, (share_x, grid_x), 1)
    column = jnp.sum(jnp.where(spot == along, symbols[:, :at_y], 0.0), axis=1, keepdims=True)
    for i in range(share_x):
        symbol = column[i : i + 1] + plane
        fac[pl.ds(i * part_y, part_y), :] = (1.0 - 0.2 * symbol) / (1.0 + 0.2 * symbol)

    def along_y(blocks, base, size, i, pair, count):
        lines = jnp.concatenate(
            [
                jnp.concatenate(
                    [blocks[pl.ds(base + (s * size + i + k) * share_y, share_y), :] for s in range(north)],
                    axis=0,
                )
                for k in range(pair)
            ],
            axis=1,
        )
        high, low = halves(lines)
        return jnp.dot(
            hy[pl.ds(0, count), :],
            jnp.concatenate([high, low, high], axis=0),
            preferred_element_type=jnp.float32,
        )

    free = max(0, len(chunks) - HELD)
    def send_deep(c):
        if ahead and c == AHEAD:
            @pl.when(d != 2)
            def _():
                for other in (deeps[0], *held):
                    deep_copy(c, other, d).start()

            deep_copy(c, deeps[1], d).start()
        elif held:
            far, side = deeps
            deep_copy(c, far, d).start()
            if c < free:
                if c in NEAR_NOW:
                    deep_copy(c, held[0], d).start()
                else:
                    pl.when(~inward)(lambda: deep_copy(c, held[0], d).start())
                deep_copy(c, side, d).start()
            else:
                pl.when(inward)(lambda: deep_copy(c, side, d).start())
        else:
            for other in deeps:
                deep_copy(c, other, d).start()

    mine = pl.ds(pl.multiple_of(d * part_y, part_y), part_y)
    tables[0].wait()
    for c in range(len(chunks)):
        north_landed(c)
        if c == 0 and rounds:
            pl.semaphore_wait(round_sem.at[rounds - 1], inner)
        start, size = chunks[c]
        for i in range(0, size, 2):
            pair = min(2, size - i)
            modes = along_y(u, start * north * share_y, size, i, pair, grid_y)
            for k in range(pair):
                v[start + i + k] = modes[:, k * lanes : (k + 1) * lanes]
        last = c == len(chunks) - 1
        send_deep(c)
        if held:
            for late in NEAR_AFTER.get(c, ()):
                pl.when(inward)(lambda late=late: deep_copy(late, held[0], d).start())
        if last and held:
            @pl.when(~inward)
            def _():
                for other in (deeps[1], *held):
                    for late in range(free, len(chunks)):
                        deep_copy(late, other, d).start()
        r[d, pl.ds(start, size)] = v[pl.ds(start, size), mine]
        if ahead and c == RELAY:
            @pl.when(d == 1)
            def _():
                ahead_down().wait_recv()
                for other in norths:
                    ahead_across(other, n).start()
                eu[ahead_rows(n), :] = ein[ahead_rows(n), :]

    if ahead:
        @pl.when(d == 1)
        def _():
            start, size = chunks[AHEAD]
            every = eu.at[ahead_rows(0, north - 1)]
            pltpu.make_async_copy(every, every, ahead_sem.at[1]).wait()
            for i in range(0, size, 2):
                pair = min(2, size - i)
                modes = along_y(eu, 0, size, i, pair, 2 * part_y)
                for k in range(pair):
                    ev[i + k] = modes[:, k * lanes : (k + 1) * lanes]
            ahead_on().start()
            r[2, pl.ds(start, size)] = ev[:, part_y:]

    tables[1].wait()
    order = list(range(len(chunks)))
    if ahead:
        order.remove(AHEAD)
        order.insert(free - 1, AHEAD)
    for c in order:
        start, size = chunks[c]
        deep_landed(c)
        if held:
            for late in NEAR_THEN.get(c, ()):
                pl.when(inward)(lambda late=late: deep_copy(late, held[0], d).start())
        parts = [r[s, pl.ds(*chunks[c])].reshape(size * part_y, lanes) for s in range(deep)]
        factor = fac[pl.ds(start * part_y, size * part_y), :]
        lines = [
            jnp.concatenate([p[:, f * share_z : (f + 1) * share_z] for p in parts], axis=1)
            for f in range(fields)
        ]
        if size == 1:
            count = fields * size * part_y
            high, low = halves(jnp.concatenate(lines, axis=0))
            both = jnp.dot(
                jnp.concatenate([high, low], axis=0),
                hz[pl.ds(0, grid_z), :],
                preferred_element_type=jnp.float32,
            )
            rest = jnp.dot(high, hz[pl.ds(2 * grid_z, grid_z), :], preferred_element_type=jnp.float32)
            modes = both[:count] + both[count:] + rest
            modes = [modes[f * size * part_y : (f + 1) * size * part_y] for f in range(fields)]
        else:
            modes = []
            for f in range(fields):
                high, low = halves(lines[f])
                modes.append(
                    jnp.dot(
                        jnp.concatenate([high, low, high], axis=1),
                        hz[...],
                        preferred_element_type=jnp.float32,
                    )
                )
        for f in range(fields):
            out[f, pl.ds(*chunks[c])] = (modes[f] * factor).reshape(size, part_y, grid_z)

    def sent(semaphore, count):
        every = wa.at[pl.ds(0, count)]
        pltpu.make_async_copy(every, every, semaphore).wait()

    across, along = (north - 1) * share_x * share_y, (deep - 1) * share_x * part_y
    sent(ns_sem.at[0], across)
    if ahead:
        extra = chunks[AHEAD][1]

        @pl.when(d == 1)
        def _():
            sent(ahead_sem.at[2], (north - 1) * extra * share_y)
            sent(ds_sem.at[0], along + extra * part_y)

        @pl.when(d == 2)
        def _():
            sent(ahead_sem.at[2], north * extra * share_y)
            sent(ds_sem.at[0], along - 2 * extra * part_y)

        @pl.when((d == 0) | (d == 3))
        def _():
            sent(ds_sem.at[0], along)
    else:
        sent(ds_sem.at[0], along)


def local(north, deep, forcing, symbol_x, symbol_y, symbol_z):
    fields, grid_x, share_y, share_z = forcing.shape
    grid_y, grid_z = symbol_y.shape[0], symbol_z.shape[0]
    share_x, part_y = grid_x // north, grid_y // deep
    chunks = chunk_starts(share_x)
    lanes = fields * share_z

    modes = np.arange(grid_x).reshape(north, share_x)
    order = np.concatenate([modes[:, start : start + size].reshape(-1) for start, size in chunks])
    high, low = table_halves(transform_table(grid_x)[order])
    split = sum(size for _, size in chunks[:EARLY]) * north
    hx = np.concatenate(
        [
            np.block([[high[part], high[part]], [low[part], np.zeros_like(low[part])]])
            for part in (slice(0, split), slice(split, grid_x))
        ],
        axis=0,
    )
    high, low = table_halves(transform_table(grid_y))
    hy = np.concatenate([high, high, low], axis=1)
    high, low = table_halves(transform_table(grid_z))
    hz = np.concatenate([high, high, low], axis=0)

    groups, extra = 1, chunks[min(AHEAD, len(chunks) - 1)][1]
    vmem = pl.BlockSpec(memory_space=pltpu.VMEM)
    buffers = [
        pltpu.VMEM((fields, share_y, share_z, grid_x), jnp.float32),
        pltpu.VMEM(hx.shape, jnp.bfloat16),
        pltpu.VMEM(hy.shape, jnp.bfloat16),
        pltpu.VMEM(hz.shape, jnp.bfloat16),
        pltpu.VMEM((grid_x * share_y, lanes), jnp.float32),
        pltpu.VMEM((grid_y * share_x, lanes), jnp.float32),
        pltpu.VMEM((share_x, grid_y, lanes), jnp.float32),
        pltpu.VMEM((deep, share_x, part_y, lanes), jnp.float32),
        pltpu.VMEM((share_x * part_y, grid_z), jnp.float32),
        pltpu.VMEM((extra * north * share_y, lanes), jnp.float32),
        pltpu.VMEM((extra * north * share_y, lanes), jnp.float32),
        pltpu.VMEM((extra, 2 * part_y, lanes), jnp.float32),
    ]
    result = fields * share_x * part_y * grid_z
    held = sum(math.prod(b.shape) * jnp.dtype(b.dtype).itemsize for b in buffers)
    return pl.pallas_call(
        functools.partial(kernel, (north, deep, chunks, min(EARLY, len(chunks)))),
        out_shape=pltpu.VMEM((fields, share_x, part_y, grid_z), jnp.float32),
        in_specs=[pl.BlockSpec(memory_space=pltpu.HBM)] * 7,
        out_specs=vmem,
        scratch_shapes=[
            pltpu.VMEM((1, grid_x + grid_y + grid_z), jnp.float32),
            *buffers,
            pltpu.SemaphoreType.DMA((groups,)),
            pltpu.SemaphoreType.DMA((4,)),
            pltpu.SemaphoreType.DMA((1,)),
            pltpu.SemaphoreType.DMA((len(chunks),)),
            pltpu.SemaphoreType.DMA((1,)),
            pltpu.SemaphoreType.DMA((len(chunks),)),
            pltpu.SemaphoreType.REGULAR((max(1, deep - 2),)),
            pltpu.SemaphoreType.DMA((3,)),
        ],
        compiler_params=pltpu.CompilerParams(
            collective_id=0, has_side_effects=True, vmem_limit_bytes=max(held + 2**23, 60 * 2**20 - 4 * result)
        ),
    )(
        forcing.transpose(0, 2, 3, 1),
        jnp.asarray(hx),
        jnp.asarray(hy),
        jnp.asarray(hz),
        symbol_x[None, :],
        symbol_y[None, :],
        symbol_z[None, :],
    )


def solution(mesh):
    placed = (P(None, None, "north", "deep"), P(), P(), P())
    return jax.shard_map(
        functools.partial(local, mesh.shape["north"], mesh.shape["deep"]),
        mesh=mesh,
        in_specs=placed,
        out_specs=P(None, "north", "deep", None),
        check_vma=False,
    )
```

```python
import functools
import math

import jax
import jax.numpy as jnp
import numpy as np
from jax import lax
from jax.experimental import pallas as pl
from jax.experimental.pallas import tpu as pltpu
from jax.sharding import PartitionSpec as P

CHUNKS = (1, 2, 1, 4, 4, 3, 1)
EARLY = 3
HELD = 3
AHEAD = 1
FEW = 2
RELAY = 3
NEAR_NOW = (0, 1, 2, 3)
NEAR_AFTER = {}
NEAR_THEN = {3: (4, 5, 6)}


def transform_table(count):
    rank = np.arange(count)
    odd = (2 * rank[:, None] + 1) * (2 * rank[None, :] + 1) % (8 * count)
    return (np.cos(np.pi / (4 * count) * odd) * np.sqrt(2.0 / count)).astype(np.float32)


def chunk_starts(share):
    unit = max(1, share // sum(CHUNKS))
    found, start = [], 0
    for weight in CHUNKS:
        size = min(unit * weight, share - start)
        if size > 0:
            found.append((start, size))
        start += size
    if start < share:
        found.append((start, share - start))
    return tuple(found)


def halves(values):
    high = values.astype(jnp.bfloat16)
    low = (values - high.astype(jnp.float32)).astype(jnp.bfloat16)
    return high, low


def table_halves(table):
    high = table.astype(jnp.bfloat16)
    low = (table - high.astype(np.float32)).astype(jnp.bfloat16)
    return high, low


def partners(me, count):
    found = []
    for step in range(count - 1, 0, -1):
        if count & (count - 1):
            found.append(lax.rem(me + step, count))
            continue
        other = me
        for bit in range(count.bit_length() - 1):
            if step >> bit & 1:
                other = other + (1 - 2 * ((me // 2**bit) % 2)) * 2**bit
        found.append(other)
    return found


def kernel(
    sizes, forcing, tx, ty, tz, gx, gy, gz, out, final, factors, hz, symbols, xin, hx, hy, wa, u, v, r, fac, ein, eu, ev,
    in_sem, table_sem, ns_sem, nr_sem, ds_sem, dr_sem, round_sem, ahead_sem,
):
    north, deep, chunks, early = sizes
    fields, share_y, share_z, grid_x = forcing.shape
    share_x, part_y = out.shape[1], out.shape[2]
    grid_y, grid_z = v.shape[1], out.shape[3]
    lanes, rounds = fields * share_z, max(0, deep - 2)
    few = min(FEW, north)
    ahead = merged = deep == 4 and len(chunks) > RELAY
    n, d = lax.axis_index("north"), lax.axis_index("deep")
    norths, deeps = partners(n, north), partners(d, deep)
    held, inward, favoured = (), (d == 1) | (d == 2), n < FEW
    patient = (d == 3) & favoured
    if deep == 4:
        far = jnp.where(d < 2, 3, 0)
        near, side = far + 1 - 2 * (far % 2), d + 1 - 2 * (d % 2)
        deeps, held = (far, side), (near,)

    first = pltpu.make_async_copy(tx, hx, table_sem.at[0])
    groups = in_sem.shape[0]
    per = share_y // groups
    loads = []
    for g in range(groups):
        part = (slice(None), pl.ds(g * per, per))
        loads.append(pltpu.make_async_copy(forcing.at[part], xin.at[part], in_sem.at[g]))
        loads[-1].start()
    first.start()

    barrier = pltpu.get_barrier_semaphore()
    inner = (d > 0).astype(jnp.int32) + (d < deep - 1).astype(jnp.int32)

    def signal_beside(semaphore):
        for other, there in ((d - 1, d > 0), (d + 1, d < deep - 1)):
            @pl.when(there)
            def _():
                pl.semaphore_signal(
                    semaphore, device_id={"deep": other}, device_id_type=pl.DeviceIdType.MESH
                )

    signal_beside(barrier)
    for other in norths:
        pl.semaphore_signal(barrier, device_id={"north": other}, device_id_type=pl.DeviceIdType.MESH)
    tables = [pltpu.make_async_copy(source, target, table_sem.at[k + 1]) for k, (source, target) in enumerate(((ty, hy), (tz, hz)))]
    pair = 2 if per % 2 == 0 else 1

    def along_x(g, start, count):
        for y in range(g * per, (g + 1) * per, pair):
            high, low = halves(
                jnp.concatenate([xin[f, y + k] for k in range(pair) for f in range(fields)], axis=0)
            )
            both = lax.dot_general(
                hx[pl.ds(2 * start, 2 * count), :],
                jnp.concatenate([high, low], axis=1),
                (((1,), (1,)), ((), ())),
                preferred_element_type=jnp.float32,
            )
            modes = both[:count] + both[count:]
            for k in range(pair):
                wa[pl.ds(start * share_y + y + k, count, stride=share_y), :] = modes[
                    :, k * lanes : (k + 1) * lanes
                ]

    def landing(c):
        return (c or RELAY) - 1 if merged else c

    def rows(c, other):
        start, size = chunks[c]
        at = (start * north + other * size) * share_y
        return pl.ds(pl.multiple_of(at, share_y), size * share_y)

    def north_copy(c, target, source):
        return pltpu.make_async_remote_copy(
            src_ref=wa.at[rows(c, target)],
            dst_ref=u.at[rows(c, source)],
            send_sem=ns_sem.at[0],
            recv_sem=nr_sem.at[min(c, len(chunks) - 2)],
            device_id={"north": target},
            device_id_type=pl.DeviceIdType.MESH,
        )

    def north_landed(c):
        size = sum(size for _, size in chunks[c:]) if c == len(chunks) - 2 else chunks[c][1]
        every = u.at[pl.ds(0, (north - 1) * size * share_y)]
        pltpu.make_async_copy(every, every, nr_sem.at[c]).wait()

    def deep_copy(c, target, source):
        return pltpu.make_async_remote_copy(
            src_ref=v.at[pl.ds(*chunks[c]), pl.ds(pl.multiple_of(target * part_y, part_y), part_y)],
            dst_ref=r.at[source, pl.ds(*chunks[c])],
            send_sem=ds_sem.at[0],
            recv_sem=dr_sem.at[landing(c)],
            device_id={"deep": target},
            device_id_type=pl.DeviceIdType.MESH,
        )

    def deep_landed(c):
        size = chunks[c][1] + (chunks[0][1] if merged and c == RELAY else 0)

        def take(count):
            every = r.at[pl.ds(0, count), pl.ds(0, size)]
            pltpu.make_async_copy(every, every, dr_sem.at[landing(c)]).wait()

        if ahead and c in (AHEAD, AHEAD + 1):
            own = (d == 1) if c == AHEAD else (d == 1) & favoured
            pl.when(own)(lambda: take(deep - 2))
            pl.when(~own)(lambda: take(deep - 1))
        else:
            take(deep - 1)

    def ahead_down():
        return pltpu.make_async_remote_copy(
            src_ref=wa.at[pl.ds(chunks[AHEAD][0] * north * share_y, ein.shape[0])],
            dst_ref=ein,
            send_sem=ds_sem.at[0],
            recv_sem=ahead_sem.at[0],
            device_id={"deep": 1},
            device_id_type=pl.DeviceIdType.MESH,
        )

    def ahead_block(k, other):
        first, block = k * north * chunks[AHEAD][1] * share_y, chunks[AHEAD + k][1] * share_y
        return pl.ds(first + pl.multiple_of(other * block, block), block)

    def ahead_across(k, target, source):
        return pltpu.make_async_remote_copy(
            src_ref=ein.at[ahead_block(k, target)],
            dst_ref=eu.at[ahead_block(k, source)],
            send_sem=ds_sem.at[0],
            recv_sem=ahead_sem.at[1],
            device_id={"north": target},
            device_id_type=pl.DeviceIdType.MESH,
        )

    def ahead_modes(k):
        (start, size), first = chunks[AHEAD + k], k * chunks[AHEAD][1]
        for i in range(0, size, 2):
            pair = min(2, size - i)
            modes = along_y(eu, k * north * chunks[AHEAD][1] * share_y, size, i, pair, 2 * part_y)
            for j in range(pair):
                ev[first + i + j] = modes[:, j * lanes : (j + 1) * lanes]
        pltpu.make_async_remote_copy(
            src_ref=ev.at[pl.ds(first, size), pl.ds(0, part_y)],
            dst_ref=r.at[2, pl.ds(start, size)],
            send_sem=ds_sem.at[0],
            recv_sem=dr_sem.at[landing(AHEAD + k)],
            device_id={"deep": 0},
            device_id_type=pl.DeviceIdType.MESH,
        ).start()
        r[2, pl.ds(start, size)] = ev[pl.ds(first, size), part_y:]

    def send_north(picked):
        for c in picked:
            for other in norths:
                north_copy(c, other, n).start()
        for c in picked:
            u[rows(c, n), :] = wa[rows(c, n), :]

    split = sum(size for _, size in chunks[:early]) * north
    first.wait()
    for g in range(groups):
        loads[g].wait()
    for g in range(groups):
        along_x(g, 0, split)
    for table in tables:
        table.start()
    at = 0
    for source in (gx, gy, gz):
        span = pl.ds(at, source.shape[1])
        pltpu.make_async_copy(source, symbols.at[:, span], table_sem.at[3]).start()
        at += source.shape[1]
    pl.semaphore_wait(barrier, north - 1 + inner)
    if ahead:
        pl.when(d == 2)(lambda: ahead_down().start())
    send_north(range(early))
    if rounds:
        signal_beside(round_sem.at[0])
    if split < grid_x:
        for g in range(groups):
            along_x(g, split, grid_x - split)
        send_north(range(early, len(chunks)))

    for k in range(rounds - 1):
        pl.semaphore_wait(round_sem.at[k], inner)
        signal_beside(round_sem.at[k + 1])
    pltpu.make_async_copy(symbols, symbols, table_sem.at[3]).wait()
    at_y, at_z = grid_x, grid_x + grid_y
    spot = lax.broadcasted_iota(jnp.int32, (part_y, grid_y), 0) + d * part_y
    along = lax.broadcasted_iota(jnp.int32, (part_y, grid_y), 1)
    column = jnp.sum(jnp.where(spot == along, symbols[:, at_y:at_z], 0.0), axis=1, keepdims=True)
    plane = column + symbols[:, at_z:]
    spot = lax.broadcasted_iota(jnp.int32, (share_x, grid_x), 0) + n * share_x
    along = lax.broadcasted_iota(jnp.int32, (share_x, grid_x), 1)
    column = jnp.sum(jnp.where(spot == along, symbols[:, :at_y], 0.0), axis=1, keepdims=True)
    for i in range(share_x):
        symbol = column[i : i + 1] + plane
        fac[pl.ds(i * part_y, part_y), :] = (1.0 - 0.2 * symbol) / (1.0 + 0.2 * symbol)

    def along_y(blocks, base, size, i, pair, count):
        lines = jnp.concatenate(
            [
                jnp.concatenate(
                    [blocks[pl.ds(base + (s * size + i + k) * share_y, share_y), :] for s in range(north)],
                    axis=0,
                )
                for k in range(pair)
            ],
            axis=1,
        )
        high, low = halves(lines)
        return jnp.dot(
            hy[pl.ds(0, count), :],
            jnp.concatenate([high, low, high], axis=0),
            preferred_element_type=jnp.float32,
        )

    free = max(0, len(chunks) - HELD)
    def send_deep(c):
        if ahead and c in (AHEAD, AHEAD + 1):
            @pl.when((d != 2) if c == AHEAD else ((d != 2) | ~favoured))
            def _():
                for other in (deeps[0], *held):
                    deep_copy(c, other, d).start()

            deep_copy(c, deeps[1], d).start()
        elif held:
            far, side = deeps
            deep_copy(c, far, d).start()
            if c < free:
                if c == free - 1:
                    @pl.when(~patient)
                    def _():
                        deep_copy(c, held[0], d).start()
                        deep_copy(c, side, d).start()
                else:
                    deep_copy(c, held[0], d).start()
                    deep_copy(c, side, d).start()
            else:
                pl.when(inward)(lambda: deep_copy(c, side, d).start())
        else:
            for other in deeps:
                deep_copy(c, other, d).start()

    mine = pl.ds(pl.multiple_of(d * part_y, part_y), part_y)
    tables[0].wait()
    for c in range(len(chunks)):
        if c < len(chunks) - 1:
            north_landed(c)
        if c == 0 and rounds:
            pl.semaphore_wait(round_sem.at[rounds - 1], inner)
        start, size = chunks[c]
        for i in range(0, size, 2):
            pair = min(2, size - i)
            modes = along_y(u, start * north * share_y, size, i, pair, grid_y)
            for k in range(pair):
                v[start + i + k] = modes[:, k * lanes : (k + 1) * lanes]
        last = c == len(chunks) - 1
        send_deep(c)
        if held:
            for late in NEAR_AFTER.get(c, ()):
                pl.when(inward)(lambda late=late: deep_copy(late, held[0], d).start())
        if last and held:
            @pl.when(patient)
            def _():
                for other in (deeps[1], *held):
                    deep_copy(free - 1, other, d).start()

            @pl.when(~inward)
            def _():
                for late in range(free, len(chunks)):
                    for other in (*held, deeps[1]):
                        deep_copy(late, other, d).start()
        r[d, pl.ds(start, size)] = v[pl.ds(start, size), mine]
        if ahead and c == RELAY:
            @pl.when(d == 1)
            def _():
                ahead_down().wait_recv()
                for other in norths:
                    ahead_across(0, other, n).start()
                for other in range(few):
                    @pl.when(n != other)
                    def _():
                        ahead_across(1, other, n).start()

                    @pl.when(n == other)
                    def _():
                        eu[ahead_block(1, other), :] = ein[ahead_block(1, other), :]
                eu[ahead_block(0, n), :] = ein[ahead_block(0, n), :]

    if ahead:
        @pl.when(d == 1)
        def _():
            def take(size):
                every = eu.at[pl.ds(0, (north - 1) * size * share_y)]
                pltpu.make_async_copy(every, every, ahead_sem.at[1]).wait()

            pl.when(favoured)(lambda: take(chunks[AHEAD][1] + chunks[AHEAD + 1][1]))
            pl.when(~favoured)(lambda: take(chunks[AHEAD][1]))
            ahead_modes(0)
            pl.when(favoured)(lambda: ahead_modes(1))

    tables[1].wait()
    order = list(range(len(chunks)))
    if ahead:
        order = [RELAY, 0, AHEAD + 1, AHEAD, *range(RELAY + 1, len(chunks))]
    for c in order[:-1]:
        start, size = chunks[c]
        if not (merged and c == 0):
            deep_landed(c)
        if held:
            for late in NEAR_THEN.get(c, ()):
                pl.when(inward)(lambda late=late: deep_copy(late, held[0], d).start())
        parts = [r[s, pl.ds(*chunks[c])].reshape(size * part_y, lanes) for s in range(deep)]
        along_z(parts, fac[pl.ds(start * part_y, size * part_y), :], hz, out, start)
    start, size = chunks[order[-1]]
    factors[...] = fac[pl.ds(start * part_y, size * part_y), :]
    deep_landed(order[-1])
    final[...] = r[:, pl.ds(start, size)]

    def sent(semaphore, count):
        every = wa.at[pl.ds(0, count)]
        pltpu.make_async_copy(every, every, semaphore).wait()

    across, along = (north - 1) * share_x * share_y, (deep - 1) * share_x * part_y
    sent(ns_sem.at[0], across)
    if ahead:
        most, more = chunks[AHEAD][1], chunks[AHEAD + 1][1]
        for mine, count in ((favoured, more), (~favoured, 0)):
            down = ein.shape[0] - 2 * (most + count) * part_y
            over = (north - 1) * most * share_y + (few - (1 if count else 0)) * more * share_y
            pl.when((d == 1) & mine)(lambda: sent(ds_sem.at[0], along + over + (most + count) * part_y))
            pl.when((d == 2) & mine)(lambda: sent(ds_sem.at[0], along + down))
        pl.when(~inward)(lambda: sent(ds_sem.at[0], along))
    else:
        sent(ds_sem.at[0], along)


def along_z(parts, factor, hz, out, start):
    fields, _, part_y, grid_z = out.shape
    count, share_z = parts[0].shape[0], parts[0].shape[1] // fields
    size = count // part_y
    lines = [
        jnp.concatenate([p[:, f * share_z : (f + 1) * share_z] for p in parts], axis=1) for f in range(fields)
    ]
    if size == 1:
        high, low = halves(jnp.concatenate(lines, axis=0))
        both = jnp.dot(
            jnp.concatenate([high, low], axis=0), hz[pl.ds(0, grid_z), :], preferred_element_type=jnp.float32
        )
        rest = jnp.dot(high, hz[pl.ds(2 * grid_z, grid_z), :], preferred_element_type=jnp.float32)
        modes = both[: fields * count] + both[fields * count :] + rest
        modes = [modes[f * count : (f + 1) * count] for f in range(fields)]
    else:
        modes = []
        for f in range(fields):
            high, low = halves(lines[f])
            modes.append(
                jnp.dot(jnp.concatenate([high, low, high], axis=1), hz[...], preferred_element_type=jnp.float32)
            )
    for f in range(fields):
        out[f, pl.ds(start, size)] = (modes[f] * factor).reshape(size, part_y, grid_z)


def finish(done, final, factors, hz, result, rest, sem):
    fields, share_x = done.shape[:2]
    deep, size, part_y, lanes = final.shape
    ahead = share_x - size
    pieces = sem.shape[1] - 1
    cuts = [ahead * k // pieces for k in range(pieces + 1)]
    copies = []
    for k in range(pieces):
        for f in range(fields):
            part = pl.ds(cuts[k], cuts[k + 1] - cuts[k])
            copies.append(pltpu.make_async_copy(done.at[f, part], result.at[f, part], sem.at[f, k]))
    for copy in copies:
        copy.start()
    parts = [final[s].reshape(size * part_y, lanes) for s in range(deep)]
    along_z(parts, factors[...], hz, rest, 0)
    for f in range(fields):
        copies.append(pltpu.make_async_copy(rest.at[f], result.at[f, pl.ds(ahead, size)], sem.at[f, pieces]))
        copies[-1].start()
    for copy in copies:
        copy.wait()


def local(north, deep, forcing, symbol_x, symbol_y, symbol_z):
    fields, grid_x, share_y, share_z = forcing.shape
    grid_y, grid_z = symbol_y.shape[0], symbol_z.shape[0]
    share_x, part_y = grid_x // north, grid_y // deep
    chunks = chunk_starts(share_x)
    lanes = fields * share_z

    modes = np.arange(grid_x).reshape(north, share_x)
    order = np.concatenate([modes[:, start : start + size].reshape(-1) for start, size in chunks])
    high, low = table_halves(transform_table(grid_x)[order])
    split = sum(size for _, size in chunks[:EARLY]) * north
    hx = np.concatenate(
        [
            np.block([[high[part], high[part]], [low[part], np.zeros_like(low[part])]])
            for part in (slice(0, split), slice(split, grid_x))
        ],
        axis=0,
    )
    high, low = table_halves(transform_table(grid_y))
    hy = np.concatenate([high, high, low], axis=1)
    high, low = table_halves(transform_table(grid_z))
    hz = np.concatenate([high, high, low], axis=0)

    groups, ahead = 1, deep == 4 and len(chunks) > RELAY
    most, more = (chunks[min(AHEAD + k, len(chunks) - 1)][1] for k in range(2))
    vmem = pl.BlockSpec(memory_space=pltpu.VMEM)
    buffers = [
        pltpu.VMEM((fields, share_y, share_z, grid_x), jnp.float32),
        pltpu.VMEM(hx.shape, jnp.bfloat16),
        pltpu.VMEM(hy.shape, jnp.bfloat16),
        pltpu.VMEM((grid_x * share_y, lanes), jnp.float32),
        pltpu.VMEM((grid_y * share_x, lanes), jnp.float32),
        pltpu.VMEM((share_x, grid_y, lanes), jnp.float32),
        pltpu.VMEM((deep, share_x, part_y, lanes), jnp.float32),
        pltpu.VMEM((share_x * part_y, grid_z), jnp.float32),
        pltpu.VMEM(((most * north + more * min(FEW, north)) * share_y, lanes), jnp.float32),
        pltpu.VMEM(((most + more) * north * share_y, lanes), jnp.float32),
        pltpu.VMEM((most + more, 2 * part_y, lanes), jnp.float32),
    ]
    result = fields * share_x * part_y * grid_z
    held = sum(math.prod(b.shape) * jnp.dtype(b.dtype).itemsize for b in buffers)
    size = chunks[-1][1]
    done, final, factors, hz = pl.pallas_call(
        functools.partial(kernel, (north, deep, chunks, min(EARLY, len(chunks)))),
        out_shape=[
            pltpu.VMEM((fields, share_x, part_y, grid_z), jnp.float32),
            pltpu.VMEM((deep, size, part_y, lanes), jnp.float32),
            pltpu.VMEM((size * part_y, grid_z), jnp.float32),
            pltpu.VMEM(hz.shape, jnp.bfloat16),
        ],
        in_specs=[pl.BlockSpec(memory_space=pltpu.HBM)] * 7,
        out_specs=[vmem] * 4,
        scratch_shapes=[
            pltpu.VMEM((1, grid_x + grid_y + grid_z), jnp.float32),
            *buffers,
            pltpu.SemaphoreType.DMA((groups,)),
            pltpu.SemaphoreType.DMA((4,)),
            pltpu.SemaphoreType.DMA((1,)),
            pltpu.SemaphoreType.DMA((max(1, len(chunks) - 1),)),
            pltpu.SemaphoreType.DMA((1,)),
            pltpu.SemaphoreType.DMA((len(chunks) - 1 if ahead else len(chunks),)),
            pltpu.SemaphoreType.REGULAR((max(1, deep - 2),)),
            pltpu.SemaphoreType.DMA((2,)),
        ],
        compiler_params=pltpu.CompilerParams(
            collective_id=0, has_side_effects=True, vmem_limit_bytes=max(held + 2**23, 60 * 2**20 - 4 * result)
        ),
    )(
        forcing.transpose(0, 2, 3, 1),
        jnp.asarray(hx),
        jnp.asarray(hy),
        jnp.asarray(hz),
        symbol_x[None, :],
        symbol_y[None, :],
        symbol_z[None, :],
    )
    return pl.pallas_call(
        finish,
        out_shape=jax.ShapeDtypeStruct((fields, share_x, part_y, grid_z), jnp.float32),
        in_specs=[vmem] * 4,
        out_specs=pl.BlockSpec(memory_space=pltpu.HBM),
        scratch_shapes=[
            pltpu.VMEM((fields, size, part_y, grid_z), jnp.float32),
            pltpu.SemaphoreType.DMA((fields, 2)),
        ],
        compiler_params=pltpu.CompilerParams(vmem_limit_bytes=2**24),
    )(*(pltpu.with_memory_space_constraint(held, pltpu.VMEM) for held in (done, final, factors, hz)))


def solution(mesh):
    placed = (P(None, None, "north", "deep"), P(), P(), P())
    return jax.shard_map(
        functools.partial(local, mesh.shape["north"], mesh.shape["deep"]),
        mesh=mesh,
        in_specs=placed,
        out_specs=P(None, "north", "deep", None),
        check_vma=False,
    )
```

```python
import functools
import math

import jax
import jax.numpy as jnp
import numpy as np
from jax import lax
from jax.experimental import pallas as pl
from jax.experimental.pallas import tpu as pltpu
from jax.sharding import PartitionSpec as P

CHUNKS = (1, 2, 1, 4, 4, 2, 2)
EARLY = 3
HELD = 3
AHEAD = 1
FEW = 2
RELAY = 3
NEAR_NOW = (0, 1, 2, 3)
NEAR_AFTER = {}
NEAR_THEN = {3: (4, 5, 6)}


def transform_table(count):
    rank = np.arange(count)
    odd = (2 * rank[:, None] + 1) * (2 * rank[None, :] + 1) % (8 * count)
    return (np.cos(np.pi / (4 * count) * odd) * np.sqrt(2.0 / count)).astype(np.float32)


def chunk_starts(share):
    unit = max(1, share // sum(CHUNKS))
    found, start = [], 0
    for weight in CHUNKS:
        size = min(unit * weight, share - start)
        if size > 0:
            found.append((start, size))
        start += size
    if start < share:
        found.append((start, share - start))
    return tuple(found)


def halves(values):
    high = values.astype(jnp.bfloat16)
    low = (values - high.astype(jnp.float32)).astype(jnp.bfloat16)
    return high, low


def table_halves(table):
    high = table.astype(jnp.bfloat16)
    low = (table - high.astype(np.float32)).astype(jnp.bfloat16)
    return high, low


def partners(me, count):
    found = []
    for step in range(count - 1, 0, -1):
        if count & (count - 1):
            found.append(lax.rem(me + step, count))
            continue
        other = me
        for bit in range(count.bit_length() - 1):
            if step >> bit & 1:
                other = other + (1 - 2 * ((me // 2**bit) % 2)) * 2**bit
        found.append(other)
    return found


def kernel(
    sizes, forcing, tx, ty, tz, gx, gy, gz, out, final, factors, hz, symbols, xin, hx, hy, wa, u, v, r, fac, ein, eu, ev,
    in_sem, table_sem, ns_sem, nr_sem, ds_sem, dr_sem, round_sem, ahead_sem,
):
    north, deep, chunks, early = sizes
    fields, share_y, share_z, grid_x = forcing.shape
    share_x, part_y = out.shape[1], out.shape[2]
    grid_y, grid_z = v.shape[1], out.shape[3]
    lanes, rounds = fields * share_z, max(0, deep - 2)
    few = min(FEW, north)
    ahead = merged = deep == 4 and len(chunks) > RELAY
    n, d = lax.axis_index("north"), lax.axis_index("deep")
    norths, deeps = partners(n, north), partners(d, deep)
    held, inward, favoured = (), (d == 1) | (d == 2), n < FEW
    patient = (d == 3) & favoured
    if deep == 4:
        far = jnp.where(d < 2, 3, 0)
        near, side = far + 1 - 2 * (far % 2), d + 1 - 2 * (d % 2)
        deeps, held = (far, side), (near,)

    first = pltpu.make_async_copy(tx, hx, table_sem.at[0])
    groups = in_sem.shape[0]
    per = share_y // groups
    loads = []
    for g in range(groups):
        part = (slice(None), pl.ds(g * per, per))
        loads.append(pltpu.make_async_copy(forcing.at[part], xin.at[part], in_sem.at[g]))
        loads[-1].start()
    first.start()

    barrier = pltpu.get_barrier_semaphore()
    inner = (d > 0).astype(jnp.int32) + (d < deep - 1).astype(jnp.int32)

    def signal_beside(semaphore):
        for other, there in ((d - 1, d > 0), (d + 1, d < deep - 1)):
            @pl.when(there)
            def _():
                pl.semaphore_signal(
                    semaphore, device_id={"deep": other}, device_id_type=pl.DeviceIdType.MESH
                )

    signal_beside(barrier)
    for other in norths:
        pl.semaphore_signal(barrier, device_id={"north": other}, device_id_type=pl.DeviceIdType.MESH)
    tables = [pltpu.make_async_copy(source, target, table_sem.at[k + 1]) for k, (source, target) in enumerate(((ty, hy), (tz, hz)))]
    pair = 2 if per % 2 == 0 else 1

    def along_x(g, start, count):
        for y in range(g * per, (g + 1) * per, pair):
            high, low = halves(
                jnp.concatenate([xin[f, y + k] for k in range(pair) for f in range(fields)], axis=0)
            )
            both = lax.dot_general(
                hx[pl.ds(2 * start, 2 * count), :],
                jnp.concatenate([high, low], axis=1),
                (((1,), (1,)), ((), ())),
                preferred_element_type=jnp.float32,
            )
            modes = both[:count] + both[count:]
            for k in range(pair):
                wa[pl.ds(start * share_y + y + k, count, stride=share_y), :] = modes[
                    :, k * lanes : (k + 1) * lanes
                ]

    def landing(c):
        return (c or RELAY) - 1 if merged else c

    def rows(c, other):
        start, size = chunks[c]
        at = (start * north + other * size) * share_y
        return pl.ds(pl.multiple_of(at, share_y), size * share_y)

    def north_copy(c, target, source):
        return pltpu.make_async_remote_copy(
            src_ref=wa.at[rows(c, target)],
            dst_ref=u.at[rows(c, source)],
            send_sem=ns_sem.at[0],
            recv_sem=nr_sem.at[min(c, len(chunks) - 2)],
            device_id={"north": target},
            device_id_type=pl.DeviceIdType.MESH,
        )

    def north_landed(c):
        size = sum(size for _, size in chunks[c:]) if c == len(chunks) - 2 else chunks[c][1]
        every = u.at[pl.ds(0, (north - 1) * size * share_y)]
        pltpu.make_async_copy(every, every, nr_sem.at[c]).wait()

    def deep_copy(c, target, source):
        return pltpu.make_async_remote_copy(
            src_ref=v.at[pl.ds(*chunks[c]), pl.ds(pl.multiple_of(target * part_y, part_y), part_y)],
            dst_ref=r.at[source, pl.ds(*chunks[c])],
            send_sem=ds_sem.at[0],
            recv_sem=dr_sem.at[landing(c)],
            device_id={"deep": target},
            device_id_type=pl.DeviceIdType.MESH,
        )

    def deep_landed(c):
        size = chunks[c][1] + (chunks[0][1] if merged and c == RELAY else 0)

        def take(count):
            every = r.at[pl.ds(0, count), pl.ds(0, size)]
            pltpu.make_async_copy(every, every, dr_sem.at[landing(c)]).wait()

        if ahead and c in (AHEAD, AHEAD + 1):
            own = (d == 1) if c == AHEAD else (d == 1) & favoured
            pl.when(own)(lambda: take(deep - 2))
            pl.when(~own)(lambda: take(deep - 1))
        else:
            take(deep - 1)

    def ahead_down():
        return pltpu.make_async_remote_copy(
            src_ref=wa.at[pl.ds(chunks[AHEAD][0] * north * share_y, ein.shape[0])],
            dst_ref=ein,
            send_sem=ds_sem.at[0],
            recv_sem=ahead_sem.at[0],
            device_id={"deep": 1},
            device_id_type=pl.DeviceIdType.MESH,
        )

    def ahead_block(k, other):
        first, block = k * north * chunks[AHEAD][1] * share_y, chunks[AHEAD + k][1] * share_y
        return pl.ds(first + pl.multiple_of(other * block, block), block)

    def ahead_across(k, target, source):
        return pltpu.make_async_remote_copy(
            src_ref=ein.at[ahead_block(k, target)],
            dst_ref=eu.at[ahead_block(k, source)],
            send_sem=ds_sem.at[0],
            recv_sem=ahead_sem.at[1],
            device_id={"north": target},
            device_id_type=pl.DeviceIdType.MESH,
        )

    def ahead_modes(k):
        (start, size), first = chunks[AHEAD + k], k * chunks[AHEAD][1]
        for i in range(0, size, 2):
            pair = min(2, size - i)
            modes = along_y(eu, k * north * chunks[AHEAD][1] * share_y, size, i, pair, 2 * part_y)
            for j in range(pair):
                ev[first + i + j] = modes[:, j * lanes : (j + 1) * lanes]
        pltpu.make_async_remote_copy(
            src_ref=ev.at[pl.ds(first, size), pl.ds(0, part_y)],
            dst_ref=r.at[2, pl.ds(start, size)],
            send_sem=ds_sem.at[0],
            recv_sem=dr_sem.at[landing(AHEAD + k)],
            device_id={"deep": 0},
            device_id_type=pl.DeviceIdType.MESH,
        ).start()
        r[2, pl.ds(start, size)] = ev[pl.ds(first, size), part_y:]

    def send_north(picked):
        for c in picked:
            for other in norths:
                north_copy(c, other, n).start()
        for c in picked:
            u[rows(c, n), :] = wa[rows(c, n), :]

    split = sum(size for _, size in chunks[:early]) * north
    first.wait()
    for g in range(groups):
        loads[g].wait()
    for g in range(groups):
        along_x(g, 0, split)
    for table in tables:
        table.start()
    at = 0
    for source in (gx, gy, gz):
        span = pl.ds(at, source.shape[1])
        pltpu.make_async_copy(source, symbols.at[:, span], table_sem.at[3]).start()
        at += source.shape[1]
    pl.semaphore_wait(barrier, north - 1 + inner)
    if ahead:
        pl.when(d == 2)(lambda: ahead_down().start())
    send_north(range(early))
    if rounds:
        signal_beside(round_sem.at[0])
    if split < grid_x:
        for g in range(groups):
            along_x(g, split, grid_x - split)
        send_north(range(early, len(chunks)))

    for k in range(rounds - 1):
        pl.semaphore_wait(round_sem.at[k], inner)
        signal_beside(round_sem.at[k + 1])
    pltpu.make_async_copy(symbols, symbols, table_sem.at[3]).wait()
    at_y, at_z = grid_x, grid_x + grid_y
    spot = lax.broadcasted_iota(jnp.int32, (part_y, grid_y), 0) + d * part_y
    along = lax.broadcasted_iota(jnp.int32, (part_y, grid_y), 1)
    column = jnp.sum(jnp.where(spot == along, symbols[:, at_y:at_z], 0.0), axis=1, keepdims=True)
    plane = column + symbols[:, at_z:]
    spot = lax.broadcasted_iota(jnp.int32, (share_x, grid_x), 0) + n * share_x
    along = lax.broadcasted_iota(jnp.int32, (share_x, grid_x), 1)
    column = jnp.sum(jnp.where(spot == along, symbols[:, :at_y], 0.0), axis=1, keepdims=True)
    for i in range(share_x):
        symbol = column[i : i + 1] + plane
        fac[pl.ds(i * part_y, part_y), :] = (1.0 - 0.2 * symbol) / (1.0 + 0.2 * symbol)

    def along_y(blocks, base, size, i, pair, count):
        lines = jnp.concatenate(
            [
                jnp.concatenate(
                    [blocks[pl.ds(base + (s * size + i + k) * share_y, share_y), :] for s in range(north)],
                    axis=0,
                )
                for k in range(pair)
            ],
            axis=1,
        )
        high, low = halves(lines)
        return jnp.dot(
            hy[pl.ds(0, count), :],
            jnp.concatenate([high, low, high], axis=0),
            preferred_element_type=jnp.float32,
        )

    free = max(0, len(chunks) - HELD)
    def send_deep(c):
        if ahead and c in (AHEAD, AHEAD + 1):
            @pl.when((d != 2) if c == AHEAD else ((d != 2) | ~favoured))
            def _():
                for other in (deeps[0], *held):
                    deep_copy(c, other, d).start()

            deep_copy(c, deeps[1], d).start()
        elif held:
            far, side = deeps
            deep_copy(c, far, d).start()
            if c < free:
                if c == free - 1:
                    @pl.when(~patient)
                    def _():
                        deep_copy(c, held[0], d).start()
                        deep_copy(c, side, d).start()
                else:
                    deep_copy(c, held[0], d).start()
                    deep_copy(c, side, d).start()
            else:
                pl.when(inward)(lambda: deep_copy(c, side, d).start())
        else:
            for other in deeps:
                deep_copy(c, other, d).start()

    mine = pl.ds(pl.multiple_of(d * part_y, part_y), part_y)
    tables[0].wait()
    for c in range(len(chunks)):
        if c < len(chunks) - 1:
            north_landed(c)
        if c == 0 and rounds:
            pl.semaphore_wait(round_sem.at[rounds - 1], inner)
        start, size = chunks[c]
        for i in range(0, size, 2):
            pair = min(2, size - i)
            modes = along_y(u, start * north * share_y, size, i, pair, grid_y)
            for k in range(pair):
                v[start + i + k] = modes[:, k * lanes : (k + 1) * lanes]
        last = c == len(chunks) - 1
        send_deep(c)
        if held:
            for late in NEAR_AFTER.get(c, ()):
                pl.when(inward)(lambda late=late: deep_copy(late, held[0], d).start())
        if last and held:
            @pl.when(patient)
            def _():
                for other in (deeps[1], *held):
                    deep_copy(free - 1, other, d).start()

            @pl.when(~inward)
            def _():
                for late in range(free, len(chunks)):
                    for other in (*held, deeps[1]):
                        deep_copy(late, other, d).start()
        r[d, pl.ds(start, size)] = v[pl.ds(start, size), mine]
        if ahead and c == RELAY:
            @pl.when(d == 1)
            def _():
                ahead_down().wait_recv()
                for other in norths:
                    ahead_across(0, other, n).start()
                for other in range(few):
                    @pl.when(n != other)
                    def _():
                        ahead_across(1, other, n).start()

                    @pl.when(n == other)
                    def _():
                        eu[ahead_block(1, other), :] = ein[ahead_block(1, other), :]
                eu[ahead_block(0, n), :] = ein[ahead_block(0, n), :]

    if ahead:
        @pl.when(d == 1)
        def _():
            def take(size):
                every = eu.at[pl.ds(0, (north - 1) * size * share_y)]
                pltpu.make_async_copy(every, every, ahead_sem.at[1]).wait()

            pl.when(favoured)(lambda: take(chunks[AHEAD][1] + chunks[AHEAD + 1][1]))
            pl.when(~favoured)(lambda: take(chunks[AHEAD][1]))
            ahead_modes(0)
            pl.when(favoured)(lambda: ahead_modes(1))

    tables[1].wait()
    order = list(range(len(chunks)))
    if ahead:
        order = [RELAY, 0, AHEAD + 1, AHEAD, *range(RELAY + 1, len(chunks))]
    for c in order[:-1]:
        start, size = chunks[c]
        if not (merged and c == 0):
            deep_landed(c)
        if held:
            for late in NEAR_THEN.get(c, ()):
                pl.when(inward)(lambda late=late: deep_copy(late, held[0], d).start())
        parts = [r[s, pl.ds(*chunks[c])].reshape(size * part_y, lanes) for s in range(deep)]
        along_z(parts, fac[pl.ds(start * part_y, size * part_y), :], hz, out, start)
    start, size = chunks[order[-1]]
    factors[...] = fac[pl.ds(start * part_y, size * part_y), :]
    deep_landed(order[-1])
    final[...] = r[:, pl.ds(start, size)]

    def sent(semaphore, count):
        every = wa.at[pl.ds(0, count)]
        pltpu.make_async_copy(every, every, semaphore).wait()

    across, along = (north - 1) * share_x * share_y, (deep - 1) * share_x * part_y
    sent(ns_sem.at[0], across)
    if ahead:
        most, more = chunks[AHEAD][1], chunks[AHEAD + 1][1]
        for mine, count in ((favoured, more), (~favoured, 0)):
            down = ein.shape[0] - 2 * (most + count) * part_y
            over = (north - 1) * most * share_y + (few - (1 if count else 0)) * more * share_y
            pl.when((d == 1) & mine)(lambda: sent(ds_sem.at[0], along + over + (most + count) * part_y))
            pl.when((d == 2) & mine)(lambda: sent(ds_sem.at[0], along + down))
        pl.when(~inward)(lambda: sent(ds_sem.at[0], along))
    else:
        sent(ds_sem.at[0], along)


def along_z(parts, factor, hz, out, start):
    fields, _, part_y, grid_z = out.shape
    count, share_z = parts[0].shape[0], parts[0].shape[1] // fields
    size = count // part_y
    lines = [
        jnp.concatenate([p[:, f * share_z : (f + 1) * share_z] for p in parts], axis=1) for f in range(fields)
    ]
    if size <= 2:
        high, low = halves(jnp.concatenate(lines, axis=0))
        both = jnp.dot(
            jnp.concatenate([high, low], axis=0), hz[pl.ds(0, grid_z), :], preferred_element_type=jnp.float32
        )
        rest = jnp.dot(high, hz[pl.ds(2 * grid_z, grid_z), :], preferred_element_type=jnp.float32)
        modes = both[: fields * count] + both[fields * count :] + rest
        modes = [modes[f * count : (f + 1) * count] for f in range(fields)]
    else:
        modes = []
        for f in range(fields):
            high, low = halves(lines[f])
            modes.append(
                jnp.dot(jnp.concatenate([high, low, high], axis=1), hz[...], preferred_element_type=jnp.float32)
            )
    for f in range(fields):
        out[f, pl.ds(start, size)] = (modes[f] * factor).reshape(size, part_y, grid_z)


def finish(done, final, factors, hz, result, rest, sem):
    fields, share_x = done.shape[:2]
    deep, size, part_y, lanes = final.shape
    ahead = share_x - size
    pieces = sem.shape[1] - 1
    cuts = [ahead * k // pieces for k in range(pieces + 1)]
    copies = []
    for k in range(pieces):
        for f in range(fields):
            part = pl.ds(cuts[k], cuts[k + 1] - cuts[k])
            copies.append(pltpu.make_async_copy(done.at[f, part], result.at[f, part], sem.at[f, k]))
    for copy in copies:
        copy.start()
    parts = [final[s].reshape(size * part_y, lanes) for s in range(deep)]
    along_z(parts, factors[...], hz, rest, 0)
    for f in range(fields):
        copies.append(pltpu.make_async_copy(rest.at[f], result.at[f, pl.ds(ahead, size)], sem.at[f, pieces]))
        copies[-1].start()
    for copy in copies:
        copy.wait()


def local(north, deep, forcing, symbol_x, symbol_y, symbol_z):
    fields, grid_x, share_y, share_z = forcing.shape
    grid_y, grid_z = symbol_y.shape[0], symbol_z.shape[0]
    share_x, part_y = grid_x // north, grid_y // deep
    chunks = chunk_starts(share_x)
    lanes = fields * share_z

    modes = np.arange(grid_x).reshape(north, share_x)
    order = np.concatenate([modes[:, start : start + size].reshape(-1) for start, size in chunks])
    high, low = table_halves(transform_table(grid_x)[order])
    split = sum(size for _, size in chunks[:EARLY]) * north
    hx = np.concatenate(
        [
            np.block([[high[part], high[part]], [low[part], np.zeros_like(low[part])]])
            for part in (slice(0, split), slice(split, grid_x))
        ],
        axis=0,
    )
    high, low = table_halves(transform_table(grid_y))
    hy = np.concatenate([high, high, low], axis=1)
    high, low = table_halves(transform_table(grid_z))
    hz = np.concatenate([high, high, low], axis=0)

    groups, ahead = 1, deep == 4 and len(chunks) > RELAY
    most, more = (chunks[min(AHEAD + k, len(chunks) - 1)][1] for k in range(2))
    vmem = pl.BlockSpec(memory_space=pltpu.VMEM)
    buffers = [
        pltpu.VMEM((fields, share_y, share_z, grid_x), jnp.float32),
        pltpu.VMEM(hx.shape, jnp.bfloat16),
        pltpu.VMEM(hy.shape, jnp.bfloat16),
        pltpu.VMEM((grid_x * share_y, lanes), jnp.float32),
        pltpu.VMEM((grid_y * share_x, lanes), jnp.float32),
        pltpu.VMEM((share_x, grid_y, lanes), jnp.float32),
        pltpu.VMEM((deep, share_x, part_y, lanes), jnp.float32),
        pltpu.VMEM((share_x * part_y, grid_z), jnp.float32),
        pltpu.VMEM(((most * north + more * min(FEW, north)) * share_y, lanes), jnp.float32),
        pltpu.VMEM(((most + more) * north * share_y, lanes), jnp.float32),
        pltpu.VMEM((most + more, 2 * part_y, lanes), jnp.float32),
    ]
    result = fields * share_x * part_y * grid_z
    held = sum(math.prod(b.shape) * jnp.dtype(b.dtype).itemsize for b in buffers)
    size = chunks[-1][1]
    done, final, factors, hz = pl.pallas_call(
        functools.partial(kernel, (north, deep, chunks, min(EARLY, len(chunks)))),
        out_shape=[
            pltpu.VMEM((fields, share_x, part_y, grid_z), jnp.float32),
            pltpu.VMEM((deep, size, part_y, lanes), jnp.float32),
            pltpu.VMEM((size * part_y, grid_z), jnp.float32),
            pltpu.VMEM(hz.shape, jnp.bfloat16),
        ],
        in_specs=[pl.BlockSpec(memory_space=pltpu.HBM)] * 7,
        out_specs=[vmem] * 4,
        scratch_shapes=[
            pltpu.VMEM((1, grid_x + grid_y + grid_z), jnp.float32),
            *buffers,
            pltpu.SemaphoreType.DMA((groups,)),
            pltpu.SemaphoreType.DMA((4,)),
            pltpu.SemaphoreType.DMA((1,)),
            pltpu.SemaphoreType.DMA((max(1, len(chunks) - 1),)),
            pltpu.SemaphoreType.DMA((1,)),
            pltpu.SemaphoreType.DMA((len(chunks) - 1 if ahead else len(chunks),)),
            pltpu.SemaphoreType.REGULAR((max(1, deep - 2),)),
            pltpu.SemaphoreType.DMA((2,)),
        ],
        compiler_params=pltpu.CompilerParams(
            collective_id=0, has_side_effects=True, vmem_limit_bytes=max(held + 2**23, 60 * 2**20 - 4 * result)
        ),
    )(
        forcing.transpose(0, 2, 3, 1),
        jnp.asarray(hx),
        jnp.asarray(hy),
        jnp.asarray(hz),
        symbol_x[None, :],
        symbol_y[None, :],
        symbol_z[None, :],
    )
    return pl.pallas_call(
        finish,
        out_shape=jax.ShapeDtypeStruct((fields, share_x, part_y, grid_z), jnp.float32),
        in_specs=[vmem] * 4,
        out_specs=pl.BlockSpec(memory_space=pltpu.HBM),
        scratch_shapes=[
            pltpu.VMEM((fields, size, part_y, grid_z), jnp.float32),
            pltpu.SemaphoreType.DMA((fields, 2)),
        ],
        compiler_params=pltpu.CompilerParams(vmem_limit_bytes=2**24),
    )(*(pltpu.with_memory_space_constraint(held, pltpu.VMEM) for held in (done, final, factors, hz)))


def solution(mesh):
    placed = (P(None, None, "north", "deep"), P(), P(), P())
    return jax.shard_map(
        functools.partial(local, mesh.shape["north"], mesh.shape["deep"]),
        mesh=mesh,
        in_specs=placed,
        out_specs=P(None, "north", "deep", None),
        check_vma=False,
    )
```

```python
import functools
import math

import jax
import jax.numpy as jnp
import numpy as np
from jax import lax
from jax.experimental import pallas as pl
from jax.experimental.pallas import tpu as pltpu
from jax.sharding import PartitionSpec as P

CHUNKS = (1, 2, 1, 4, 4, 2, 2)
EARLY = 3
HELD = 3
AHEAD = 1
OWNERS = (((0, 8),), ((0, 3), (4, 5)))
RELAY = 3
NEAR_NOW = (0, 1, 2, 3)
NEAR_AFTER = {}
NEAR_THEN = {3: (4, 5, 6)}


def transform_table(count):
    rank = np.arange(count)
    odd = (2 * rank[:, None] + 1) * (2 * rank[None, :] + 1) % (8 * count)
    return (np.cos(np.pi / (4 * count) * odd) * np.sqrt(2.0 / count)).astype(np.float32)


def chunk_starts(share):
    unit = max(1, share // sum(CHUNKS))
    found, start = [], 0
    for weight in CHUNKS:
        size = min(unit * weight, share - start)
        if size > 0:
            found.append((start, size))
        start += size
    if start < share:
        found.append((start, share - start))
    return tuple(found)


def halves(values):
    high = values.astype(jnp.bfloat16)
    low = (values - high.astype(jnp.float32)).astype(jnp.bfloat16)
    return high, low


def table_halves(table):
    high = table.astype(jnp.bfloat16)
    low = (table - high.astype(np.float32)).astype(jnp.bfloat16)
    return high, low


def partners(me, count):
    found = []
    for step in range(count - 1, 0, -1):
        if count & (count - 1):
            found.append(lax.rem(me + step, count))
            continue
        other = me
        for bit in range(count.bit_length() - 1):
            if step >> bit & 1:
                other = other + (1 - 2 * ((me // 2**bit) % 2)) * 2**bit
        found.append(other)
    return found


def kernel(
    sizes, forcing, tx, ty, tz, gx, gy, gz, out, final, factors, hz, symbols, xin, hx, hy, wa, u, v, r, fac, ein, eu, ev,
    in_sem, table_sem, ns_sem, nr_sem, ds_sem, dr_sem, round_sem, ahead_sem,
):
    north, deep, chunks, early = sizes
    fields, share_y, share_z, grid_x = forcing.shape
    share_x, part_y = out.shape[1], out.shape[2]
    grid_y, grid_z = v.shape[1], out.shape[3]
    lanes, rounds = fields * share_z, max(0, deep - 2)
    ahead = merged = deep == 4 and len(chunks) > RELAY
    if ahead:
        spans = [[(low, min(high, north)) for low, high in part if low < north] for part in OWNERS]
        owners = [[other for low, high in part for other in range(low, high)] for part in spans]
        sent_ahead = sum(len(owners[k]) * chunks[AHEAD + k][1] * share_y for k in range(2))
    n, d = lax.axis_index("north"), lax.axis_index("deep")
    norths, deeps = partners(n, north), partners(d, deep)
    held, inward, favoured = (), (d == 1) | (d == 2), n < 2
    if ahead:
        member = [functools.reduce(lambda a, b: a | b, [(n >= low) & (n < high) for low, high in part]) for part in spans]
        cases = (
            (member[0] & member[1], (0, 1)),
            (member[0] & ~member[1], (0,)),
            (~member[0] & member[1], (1,)),
            (~member[0] & ~member[1], ()),
        )
    patient = (d == 3) & favoured
    if deep == 4:
        far = jnp.where(d < 2, 3, 0)
        near, side = far + 1 - 2 * (far % 2), d + 1 - 2 * (d % 2)
        deeps, held = (far, side), (near,)

    first = pltpu.make_async_copy(tx, hx, table_sem.at[0])
    groups = in_sem.shape[0]
    per = share_y // groups
    loads = []
    for g in range(groups):
        part = (slice(None), pl.ds(g * per, per))
        loads.append(pltpu.make_async_copy(forcing.at[part], xin.at[part], in_sem.at[g]))
        loads[-1].start()
    first.start()

    barrier = pltpu.get_barrier_semaphore()
    inner = (d > 0).astype(jnp.int32) + (d < deep - 1).astype(jnp.int32)

    def signal_beside(semaphore):
        for other, there in ((d - 1, d > 0), (d + 1, d < deep - 1)):
            @pl.when(there)
            def _():
                pl.semaphore_signal(
                    semaphore, device_id={"deep": other}, device_id_type=pl.DeviceIdType.MESH
                )

    signal_beside(barrier)
    for other in norths:
        pl.semaphore_signal(barrier, device_id={"north": other}, device_id_type=pl.DeviceIdType.MESH)
    tables = [pltpu.make_async_copy(source, target, table_sem.at[k + 1]) for k, (source, target) in enumerate(((ty, hy), (tz, hz)))]
    pair = 2 if per % 2 == 0 else 1

    def along_x(g, start, count):
        for y in range(g * per, (g + 1) * per, pair):
            high, low = halves(
                jnp.concatenate([xin[f, y + k] for k in range(pair) for f in range(fields)], axis=0)
            )
            both = lax.dot_general(
                hx[pl.ds(2 * start, 2 * count), :],
                jnp.concatenate([high, low], axis=1),
                (((1,), (1,)), ((), ())),
                preferred_element_type=jnp.float32,
            )
            modes = both[:count] + both[count:]
            for k in range(pair):
                wa[pl.ds(start * share_y + y + k, count, stride=share_y), :] = modes[
                    :, k * lanes : (k + 1) * lanes
                ]

    def landing(c):
        return (c or RELAY) - 1 if merged else c

    def rows(c, other):
        start, size = chunks[c]
        at = (start * north + other * size) * share_y
        return pl.ds(pl.multiple_of(at, share_y), size * share_y)

    def north_copy(c, target, source):
        return pltpu.make_async_remote_copy(
            src_ref=wa.at[rows(c, target)],
            dst_ref=u.at[rows(c, source)],
            send_sem=ns_sem.at[0],
            recv_sem=nr_sem.at[min(c, len(chunks) - 2)],
            device_id={"north": target},
            device_id_type=pl.DeviceIdType.MESH,
        )

    def north_landed(c):
        size = sum(size for _, size in chunks[c:]) if c == len(chunks) - 2 else chunks[c][1]
        every = u.at[pl.ds(0, (north - 1) * size * share_y)]
        pltpu.make_async_copy(every, every, nr_sem.at[c]).wait()

    def deep_copy(c, target, source):
        return pltpu.make_async_remote_copy(
            src_ref=v.at[pl.ds(*chunks[c]), pl.ds(pl.multiple_of(target * part_y, part_y), part_y)],
            dst_ref=r.at[source, pl.ds(*chunks[c])],
            send_sem=ds_sem.at[0],
            recv_sem=dr_sem.at[landing(c)],
            device_id={"deep": target},
            device_id_type=pl.DeviceIdType.MESH,
        )

    def deep_landed(c):
        size = chunks[c][1] + (chunks[0][1] if merged and c == RELAY else 0)

        def take(count):
            every = r.at[pl.ds(0, count), pl.ds(0, size)]
            pltpu.make_async_copy(every, every, dr_sem.at[landing(c)]).wait()

        if ahead and c in (AHEAD, AHEAD + 1):
            own = (d == 1) & member[c - AHEAD]
            pl.when(own)(lambda: take(deep - 2))
            pl.when(~own)(lambda: take(deep - 1))
        else:
            take(deep - 1)

    def ahead_down():
        found = []
        for k in range(2):
            start, size = chunks[AHEAD + k]
            block, base = size * share_y, k * north * chunks[AHEAD][1] * share_y
            for low, high in spans[k]:
                part = pl.ds(low * block, (high - low) * block)
                found.append(
                    pltpu.make_async_remote_copy(
                        src_ref=wa.at[pl.ds(start * north * share_y + part.start, part.size)],
                        dst_ref=ein.at[pl.ds(base + part.start, part.size)],
                        send_sem=ds_sem.at[0],
                        recv_sem=ahead_sem.at[0],
                        device_id={"deep": 1},
                        device_id_type=pl.DeviceIdType.MESH,
                    )
                )
        return found

    def ahead_block(k, other):
        first, block = k * north * chunks[AHEAD][1] * share_y, chunks[AHEAD + k][1] * share_y
        return pl.ds(first + pl.multiple_of(other * block, block), block)

    def ahead_across(k, target, source):
        return pltpu.make_async_remote_copy(
            src_ref=ein.at[ahead_block(k, target)],
            dst_ref=eu.at[ahead_block(k, source)],
            send_sem=ds_sem.at[0],
            recv_sem=ahead_sem.at[1],
            device_id={"north": target},
            device_id_type=pl.DeviceIdType.MESH,
        )

    def ahead_modes(k):
        (start, size), first = chunks[AHEAD + k], k * chunks[AHEAD][1]
        for i in range(0, size, 2):
            pair = min(2, size - i)
            modes = along_y(eu, k * north * chunks[AHEAD][1] * share_y, size, i, pair, 2 * part_y)
            for j in range(pair):
                ev[first + i + j] = modes[:, j * lanes : (j + 1) * lanes]
        pltpu.make_async_remote_copy(
            src_ref=ev.at[pl.ds(first, size), pl.ds(0, part_y)],
            dst_ref=r.at[2, pl.ds(start, size)],
            send_sem=ds_sem.at[0],
            recv_sem=dr_sem.at[landing(AHEAD + k)],
            device_id={"deep": 0},
            device_id_type=pl.DeviceIdType.MESH,
        ).start()
        r[2, pl.ds(start, size)] = ev[pl.ds(first, size), part_y:]

    def send_north(picked):
        for c in picked:
            for other in norths:
                north_copy(c, other, n).start()
        for c in picked:
            u[rows(c, n), :] = wa[rows(c, n), :]

    split = sum(size for _, size in chunks[:early]) * north
    first.wait()
    for g in range(groups):
        loads[g].wait()
    for g in range(groups):
        along_x(g, 0, split)
    for table in tables:
        table.start()
    at = 0
    for source in (gx, gy, gz):
        span = pl.ds(at, source.shape[1])
        pltpu.make_async_copy(source, symbols.at[:, span], table_sem.at[3]).start()
        at += source.shape[1]
    pl.semaphore_wait(barrier, north - 1 + inner)
    if ahead:
        @pl.when(d == 2)
        def _():
            for copy in ahead_down():
                copy.start()

    send_north(range(early))
    if rounds:
        signal_beside(round_sem.at[0])
    if split < grid_x:
        for g in range(groups):
            along_x(g, split, grid_x - split)
        send_north(range(early, len(chunks)))

    for k in range(rounds - 1):
        pl.semaphore_wait(round_sem.at[k], inner)
        signal_beside(round_sem.at[k + 1])
    pltpu.make_async_copy(symbols, symbols, table_sem.at[3]).wait()
    at_y, at_z = grid_x, grid_x + grid_y
    spot = lax.broadcasted_iota(jnp.int32, (part_y, grid_y), 0) + d * part_y
    along = lax.broadcasted_iota(jnp.int32, (part_y, grid_y), 1)
    column = jnp.sum(jnp.where(spot == along, symbols[:, at_y:at_z], 0.0), axis=1, keepdims=True)
    plane = column + symbols[:, at_z:]
    spot = lax.broadcasted_iota(jnp.int32, (share_x, grid_x), 0) + n * share_x
    along = lax.broadcasted_iota(jnp.int32, (share_x, grid_x), 1)
    column = jnp.sum(jnp.where(spot == along, symbols[:, :at_y], 0.0), axis=1, keepdims=True)
    for i in range(share_x):
        symbol = column[i : i + 1] + plane
        fac[pl.ds(i * part_y, part_y), :] = (1.0 - 0.2 * symbol) / (1.0 + 0.2 * symbol)

    def along_y(blocks, base, size, i, pair, count):
        lines = jnp.concatenate(
            [
                jnp.concatenate(
                    [blocks[pl.ds(base + (s * size + i + k) * share_y, share_y), :] for s in range(north)],
                    axis=0,
                )
                for k in range(pair)
            ],
            axis=1,
        )
        high, low = halves(lines)
        return jnp.dot(
            hy[pl.ds(0, count), :],
            jnp.concatenate([high, low, high], axis=0),
            preferred_element_type=jnp.float32,
        )

    free = max(0, len(chunks) - HELD)
    def send_deep(c):
        if ahead and c in (AHEAD, AHEAD + 1):
            @pl.when((d != 2) | ~member[c - AHEAD])
            def _():
                for other in (deeps[0], *held):
                    deep_copy(c, other, d).start()

            deep_copy(c, deeps[1], d).start()
        elif held:
            far, side = deeps
            deep_copy(c, far, d).start()
            if c < free:
                if c == free - 1:
                    @pl.when(~patient)
                    def _():
                        deep_copy(c, held[0], d).start()
                        deep_copy(c, side, d).start()
                else:
                    deep_copy(c, held[0], d).start()
                    deep_copy(c, side, d).start()
            else:
                pl.when(inward)(lambda: deep_copy(c, side, d).start())
        else:
            for other in deeps:
                deep_copy(c, other, d).start()

    mine = pl.ds(pl.multiple_of(d * part_y, part_y), part_y)
    tables[0].wait()
    for c in range(len(chunks)):
        if c < len(chunks) - 1:
            north_landed(c)
        if c == 0 and rounds:
            pl.semaphore_wait(round_sem.at[rounds - 1], inner)
        start, size = chunks[c]
        for i in range(0, size, 2):
            pair = min(2, size - i)
            modes = along_y(u, start * north * share_y, size, i, pair, grid_y)
            for k in range(pair):
                v[start + i + k] = modes[:, k * lanes : (k + 1) * lanes]
        last = c == len(chunks) - 1
        send_deep(c)
        if held:
            for late in NEAR_AFTER.get(c, ()):
                pl.when(inward)(lambda late=late: deep_copy(late, held[0], d).start())
        if last and held:
            @pl.when(patient)
            def _():
                for other in (deeps[1], *held):
                    deep_copy(free - 1, other, d).start()

            @pl.when(~inward)
            def _():
                for late in range(free, len(chunks)):
                    for other in (*held, deeps[1]):
                        deep_copy(late, other, d).start()
        r[d, pl.ds(start, size)] = v[pl.ds(start, size), mine]
        if ahead and c == RELAY:
            @pl.when(d == 1)
            def _():
                every = ein.at[pl.ds(0, sent_ahead)]
                pltpu.make_async_copy(every, every, ahead_sem.at[0]).wait()
                for k in range(2):
                    for other in owners[k]:
                        @pl.when(n != other)
                        def _():
                            ahead_across(k, other, n).start()

                        @pl.when(n == other)
                        def _():
                            eu[ahead_block(k, other), :] = ein[ahead_block(k, other), :]

    if ahead:
        @pl.when(d == 1)
        def _():
            for mine, picked in cases:
                if picked:
                    def take():
                        size = sum(chunks[AHEAD + k][1] for k in picked)
                        every = eu.at[pl.ds(0, (north - 1) * size * share_y)]
                        pltpu.make_async_copy(every, every, ahead_sem.at[1]).wait()

                    pl.when(mine)(take)
            for k in range(2):
                pl.when(member[k])(lambda: ahead_modes(k))

    tables[1].wait()
    order = list(range(len(chunks)))
    if ahead:
        order = [RELAY, 0, AHEAD + 1, AHEAD, *range(RELAY + 1, len(chunks))]
    for c in order[:-1]:
        start, size = chunks[c]
        if not (merged and c == 0):
            deep_landed(c)
        if held:
            for late in NEAR_THEN.get(c, ()):
                pl.when(inward)(lambda late=late: deep_copy(late, held[0], d).start())
        parts = [r[s, pl.ds(*chunks[c])].reshape(size * part_y, lanes) for s in range(deep)]
        along_z(parts, fac[pl.ds(start * part_y, size * part_y), :], hz, out, start)
    start, size = chunks[order[-1]]
    factors[...] = fac[pl.ds(start * part_y, size * part_y), :]
    deep_landed(order[-1])
    final[...] = r[:, pl.ds(start, size)]

    def sent(semaphore, count):
        every = wa.at[pl.ds(0, count)]
        pltpu.make_async_copy(every, every, semaphore).wait()

    across, along = (north - 1) * share_x * share_y, (deep - 1) * share_x * part_y
    sent(ns_sem.at[0], across)
    if ahead:
        for mine, picked in cases:
            own = sum(chunks[AHEAD + k][1] for k in picked)
            over = sent_ahead - own * share_y + own * part_y
            down = sent_ahead - 2 * own * part_y
            pl.when((d == 1) & mine)(lambda: sent(ds_sem.at[0], along + over))
            pl.when((d == 2) & mine)(lambda: sent(ds_sem.at[0], along + down))
        pl.when(~inward)(lambda: sent(ds_sem.at[0], along))
    else:
        sent(ds_sem.at[0], along)


def along_z(parts, factor, hz, out, start):
    fields, _, part_y, grid_z = out.shape
    count, share_z = parts[0].shape[0], parts[0].shape[1] // fields
    size = count // part_y
    lines = [
        jnp.concatenate([p[:, f * share_z : (f + 1) * share_z] for p in parts], axis=1) for f in range(fields)
    ]
    if size <= 2:
        high, low = halves(jnp.concatenate(lines, axis=0))
        both = jnp.dot(
            jnp.concatenate([high, low], axis=0), hz[pl.ds(0, grid_z), :], preferred_element_type=jnp.float32
        )
        rest = jnp.dot(high, hz[pl.ds(2 * grid_z, grid_z), :], preferred_element_type=jnp.float32)
        modes = both[: fields * count] + both[fields * count :] + rest
        modes = [modes[f * count : (f + 1) * count] for f in range(fields)]
    else:
        modes = []
        for f in range(fields):
            high, low = halves(lines[f])
            modes.append(
                jnp.dot(jnp.concatenate([high, low, high], axis=1), hz[...], preferred_element_type=jnp.float32)
            )
    for f in range(fields):
        out[f, pl.ds(start, size)] = (modes[f] * factor).reshape(size, part_y, grid_z)


def finish(done, final, factors, hz, result, rest, sem):
    fields, share_x = done.shape[:2]
    deep, size, part_y, lanes = final.shape
    ahead = share_x - size
    bulk = pltpu.make_async_copy(done.at[:, pl.ds(0, ahead)], result.at[:, pl.ds(0, ahead)], sem.at[0])
    bulk.start()
    parts = [final[s].reshape(size * part_y, lanes) for s in range(deep)]
    along_z(parts, factors[...], hz, rest, 0)
    last = pltpu.make_async_copy(rest, result.at[:, pl.ds(ahead, size)], sem.at[1])
    last.start()
    bulk.wait()
    last.wait()


def local(north, deep, forcing, symbol_x, symbol_y, symbol_z):
    fields, grid_x, share_y, share_z = forcing.shape
    grid_y, grid_z = symbol_y.shape[0], symbol_z.shape[0]
    share_x, part_y = grid_x // north, grid_y // deep
    chunks = chunk_starts(share_x)
    lanes = fields * share_z

    modes = np.arange(grid_x).reshape(north, share_x)
    order = np.concatenate([modes[:, start : start + size].reshape(-1) for start, size in chunks])
    high, low = table_halves(transform_table(grid_x)[order])
    split = sum(size for _, size in chunks[:EARLY]) * north
    hx = np.concatenate(
        [
            np.block([[high[part], high[part]], [low[part], np.zeros_like(low[part])]])
            for part in (slice(0, split), slice(split, grid_x))
        ],
        axis=0,
    )
    high, low = table_halves(transform_table(grid_y))
    hy = np.concatenate([high, high, low], axis=1)
    high, low = table_halves(transform_table(grid_z))
    hz = np.concatenate([high, high, low], axis=0)

    groups, ahead = 1, deep == 4 and len(chunks) > RELAY
    most, more = (chunks[min(AHEAD + k, len(chunks) - 1)][1] for k in range(2))
    vmem = pl.BlockSpec(memory_space=pltpu.VMEM)
    buffers = [
        pltpu.VMEM((fields, share_y, share_z, grid_x), jnp.float32),
        pltpu.VMEM(hx.shape, jnp.bfloat16),
        pltpu.VMEM(hy.shape, jnp.bfloat16),
        pltpu.VMEM((grid_x * share_y, lanes), jnp.float32),
        pltpu.VMEM((grid_y * share_x, lanes), jnp.float32),
        pltpu.VMEM((share_x, grid_y, lanes), jnp.float32),
        pltpu.VMEM((deep, share_x, part_y, lanes), jnp.float32),
        pltpu.VMEM((share_x * part_y, grid_z), jnp.float32),
        pltpu.VMEM(((most + more) * north * share_y, lanes), jnp.float32),
        pltpu.VMEM(((most + more) * north * share_y, lanes), jnp.float32),
        pltpu.VMEM((most + more, 2 * part_y, lanes), jnp.float32),
    ]
    result = fields * share_x * part_y * grid_z
    held = sum(math.prod(b.shape) * jnp.dtype(b.dtype).itemsize for b in buffers)
    size = chunks[-1][1]
    done, final, factors, hz = pl.pallas_call(
        functools.partial(kernel, (north, deep, chunks, min(EARLY, len(chunks)))),
        out_shape=[
            pltpu.VMEM((fields, share_x, part_y, grid_z), jnp.float32),
            pltpu.VMEM((deep, size, part_y, lanes), jnp.float32),
            pltpu.VMEM((size * part_y, grid_z), jnp.float32),
            pltpu.VMEM(hz.shape, jnp.bfloat16),
        ],
        in_specs=[pl.BlockSpec(memory_space=pltpu.HBM)] * 7,
        out_specs=[vmem] * 4,
        scratch_shapes=[
            pltpu.VMEM((1, grid_x + grid_y + grid_z), jnp.float32),
            *buffers,
            pltpu.SemaphoreType.DMA((groups,)),
            pltpu.SemaphoreType.DMA((4,)),
            pltpu.SemaphoreType.DMA((1,)),
            pltpu.SemaphoreType.DMA((max(1, len(chunks) - 1),)),
            pltpu.SemaphoreType.DMA((1,)),
            pltpu.SemaphoreType.DMA((len(chunks) - 1 if ahead else len(chunks),)),
            pltpu.SemaphoreType.REGULAR((max(1, deep - 2),)),
            pltpu.SemaphoreType.DMA((2,)),
        ],
        compiler_params=pltpu.CompilerParams(
            collective_id=0, has_side_effects=True, vmem_limit_bytes=max(held + 2**23, 60 * 2**20 - 4 * result)
        ),
    )(
        forcing.transpose(0, 2, 3, 1),
        jnp.asarray(hx),
        jnp.asarray(hy),
        jnp.asarray(hz),
        symbol_x[None, :],
        symbol_y[None, :],
        symbol_z[None, :],
    )
    return pl.pallas_call(
        finish,
        out_shape=jax.ShapeDtypeStruct((fields, share_x, part_y, grid_z), jnp.float32),
        in_specs=[vmem] * 4,
        out_specs=pl.BlockSpec(memory_space=pltpu.HBM),
        scratch_shapes=[
            pltpu.VMEM((fields, size, part_y, grid_z), jnp.float32),
            pltpu.SemaphoreType.DMA((2,)),
        ],
        compiler_params=pltpu.CompilerParams(vmem_limit_bytes=2**24),
    )(*(pltpu.with_memory_space_constraint(held, pltpu.VMEM) for held in (done, final, factors, hz)))


def solution(mesh):
    placed = (P(None, None, "north", "deep"), P(), P(), P())
    return jax.shard_map(
        functools.partial(local, mesh.shape["north"], mesh.shape["deep"]),
        mesh=mesh,
        in_specs=placed,
        out_specs=P(None, "north", "deep", None),
        check_vma=False,
    )
```

```python
import functools
import math

import jax
import jax.numpy as jnp
import numpy as np
from jax import lax
from jax.experimental import pallas as pl
from jax.experimental.pallas import tpu as pltpu
from jax.sharding import PartitionSpec as P

CHUNKS = (1, 2, 1, 4, 4, 2, 2)
EARLY = 3
HELD = 3
AHEAD = 1
OWNERS = (((0, 8),), ((1, 2), (3, 4), (5, 6), (7, 8)))
RELAY = 3
NEAR_NOW = (0, 1, 2, 3)
NEAR_AFTER = {6: (4, 5, 6)}
NEAR_THEN = {3: (4, 5, 6)}


def transform_table(count):
    rank = np.arange(count)
    odd = (2 * rank[:, None] + 1) * (2 * rank[None, :] + 1) % (8 * count)
    return (np.cos(np.pi / (4 * count) * odd) * np.sqrt(2.0 / count)).astype(np.float32)


def chunk_starts(share):
    unit = max(1, share // sum(CHUNKS))
    found, start = [], 0
    for weight in CHUNKS:
        size = min(unit * weight, share - start)
        if size > 0:
            found.append((start, size))
        start += size
    if start < share:
        found.append((start, share - start))
    return tuple(found)


def halves(values):
    high = values.astype(jnp.bfloat16)
    low = (values - high.astype(jnp.float32)).astype(jnp.bfloat16)
    return high, low


def table_halves(table):
    high = table.astype(jnp.bfloat16)
    low = (table - high.astype(np.float32)).astype(jnp.bfloat16)
    return high, low


def partners(me, count):
    found = []
    for step in range(count - 1, 0, -1):
        if count & (count - 1):
            found.append(lax.rem(me + step, count))
            continue
        other = me
        for bit in range(count.bit_length() - 1):
            if step >> bit & 1:
                other = other + (1 - 2 * ((me // 2**bit) % 2)) * 2**bit
        found.append(other)
    return found


def kernel(
    sizes, forcing, tx, ty, tz, gx, gy, gz, out, final, factors, hz, symbols, xin, hx, hy, wa, u, v, r, fac, ein, eu, ev,
    in_sem, table_sem, ns_sem, nr_sem, ds_sem, dr_sem, round_sem, ahead_sem,
):
    north, deep, chunks, early = sizes
    fields, share_y, share_z, grid_x = forcing.shape
    share_x, part_y = out.shape[1], out.shape[2]
    grid_y, grid_z = v.shape[1], out.shape[3]
    lanes, rounds = fields * share_z, max(0, deep - 2)
    ahead = merged = deep == 4 and len(chunks) > RELAY
    if ahead:
        spans = [[(low, min(high, north)) for low, high in part if low < north] for part in OWNERS]
        owners = [[other for low, high in part for other in range(low, high)] for part in spans]
        sent_ahead = sum(len(owners[k]) * chunks[AHEAD + k][1] * share_y for k in range(2))
    n, d = lax.axis_index("north"), lax.axis_index("deep")
    norths, deeps = partners(n, north), partners(d, deep)
    evens = norths
    if north % 2 == 0 and north & (north - 1) == 0:
        chips = partners(n // 2, north // 2)
        evens = [2 * chip for chip in chips] + [2 * chip + 1 for chip in chips] + norths[-1:]
    held, inward, favoured = (), (d == 1) | (d == 2), n < 2
    if ahead:
        member = [functools.reduce(lambda a, b: a | b, [(n >= low) & (n < high) for low, high in part]) for part in spans]
        cases = (
            (member[0] & member[1], (0, 1)),
            (member[0] & ~member[1], (0,)),
            (~member[0] & member[1], (1,)),
            (~member[0] & ~member[1], ()),
        )
    patient = (d == 3) & favoured
    if deep == 4:
        far = jnp.where(d < 2, 3, 0)
        near, side = far + 1 - 2 * (far % 2), d + 1 - 2 * (d % 2)
        deeps, held = (far, side), (near,)

    first = pltpu.make_async_copy(tx, hx, table_sem.at[0])
    groups = in_sem.shape[0]
    per = share_y // groups
    loads = []
    for g in range(groups):
        part = (slice(None), pl.ds(g * per, per))
        loads.append(pltpu.make_async_copy(forcing.at[part], xin.at[part], in_sem.at[g]))
        loads[-1].start()
    first.start()

    barrier = pltpu.get_barrier_semaphore()
    inner = (d > 0).astype(jnp.int32) + (d < deep - 1).astype(jnp.int32)

    def signal_beside(semaphore):
        for other, there in ((d - 1, d > 0), (d + 1, d < deep - 1)):
            @pl.when(there)
            def _():
                pl.semaphore_signal(
                    semaphore, device_id={"deep": other}, device_id_type=pl.DeviceIdType.MESH
                )

    signal_beside(barrier)
    for other in norths:
        pl.semaphore_signal(barrier, device_id={"north": other}, device_id_type=pl.DeviceIdType.MESH)
    tables = [pltpu.make_async_copy(source, target, table_sem.at[k + 1]) for k, (source, target) in enumerate(((ty, hy), (tz, hz)))]
    pair = 2 if per % 2 == 0 else 1

    def along_x(g, start, count):
        for y in range(g * per, (g + 1) * per, pair):
            high, low = halves(
                jnp.concatenate([xin[f, y + k] for k in range(pair) for f in range(fields)], axis=0)
            )
            both = lax.dot_general(
                hx[pl.ds(2 * start, 2 * count), :],
                jnp.concatenate([high, low], axis=1),
                (((1,), (1,)), ((), ())),
                preferred_element_type=jnp.float32,
            )
            modes = both[:count] + both[count:]
            for k in range(pair):
                wa[pl.ds(start * share_y + y + k, count, stride=share_y), :] = modes[
                    :, k * lanes : (k + 1) * lanes
                ]

    def landing(c):
        return (c or RELAY) - 1 if merged else c

    def rows(c, other):
        start, size = chunks[c]
        at = (start * north + other * size) * share_y
        return pl.ds(pl.multiple_of(at, share_y), size * share_y)

    def north_copy(c, target, source):
        return pltpu.make_async_remote_copy(
            src_ref=wa.at[rows(c, target)],
            dst_ref=u.at[rows(c, source)],
            send_sem=ns_sem.at[0],
            recv_sem=nr_sem.at[min(c, len(chunks) - 2)],
            device_id={"north": target},
            device_id_type=pl.DeviceIdType.MESH,
        )

    def north_landed(c):
        size = sum(size for _, size in chunks[c:]) if c == len(chunks) - 2 else chunks[c][1]
        every = u.at[pl.ds(0, (north - 1) * size * share_y)]
        pltpu.make_async_copy(every, every, nr_sem.at[c]).wait()

    def deep_copy(c, target, source):
        return pltpu.make_async_remote_copy(
            src_ref=v.at[pl.ds(*chunks[c]), pl.ds(pl.multiple_of(target * part_y, part_y), part_y)],
            dst_ref=r.at[source, pl.ds(*chunks[c])],
            send_sem=ds_sem.at[0],
            recv_sem=dr_sem.at[landing(c)],
            device_id={"deep": target},
            device_id_type=pl.DeviceIdType.MESH,
        )

    def deep_landed(c):
        size = chunks[c][1] + (chunks[0][1] if merged and c == RELAY else 0)

        def take(count):
            every = r.at[pl.ds(0, count), pl.ds(0, size)]
            pltpu.make_async_copy(every, every, dr_sem.at[landing(c)]).wait()

        if ahead and c in (AHEAD, AHEAD + 1):
            own = (d == 1) & member[c - AHEAD]
            pl.when(own)(lambda: take(deep - 2))
            pl.when(~own)(lambda: take(deep - 1))
        else:
            take(deep - 1)

    def ahead_down():
        found = []
        for k in range(2):
            start, size = chunks[AHEAD + k]
            block, base = size * share_y, k * north * chunks[AHEAD][1] * share_y
            for low, high in spans[k]:
                part = pl.ds(low * block, (high - low) * block)
                found.append(
                    pltpu.make_async_remote_copy(
                        src_ref=wa.at[pl.ds(start * north * share_y + part.start, part.size)],
                        dst_ref=ein.at[pl.ds(base + part.start, part.size)],
                        send_sem=ds_sem.at[0],
                        recv_sem=ahead_sem.at[0],
                        device_id={"deep": 1},
                        device_id_type=pl.DeviceIdType.MESH,
                    )
                )
        return found

    def ahead_block(k, other):
        first, block = k * north * chunks[AHEAD][1] * share_y, chunks[AHEAD + k][1] * share_y
        return pl.ds(first + pl.multiple_of(other * block, block), block)

    def ahead_across(k, target, source):
        return pltpu.make_async_remote_copy(
            src_ref=ein.at[ahead_block(k, target)],
            dst_ref=eu.at[ahead_block(k, source)],
            send_sem=ds_sem.at[0],
            recv_sem=ahead_sem.at[1],
            device_id={"north": target},
            device_id_type=pl.DeviceIdType.MESH,
        )

    def ahead_modes(k):
        (start, size), first = chunks[AHEAD + k], k * chunks[AHEAD][1]
        for i in range(0, size, 2):
            pair = min(2, size - i)
            modes = along_y(eu, k * north * chunks[AHEAD][1] * share_y, size, i, pair, 2 * part_y)
            for j in range(pair):
                ev[first + i + j] = modes[:, j * lanes : (j + 1) * lanes]
        pltpu.make_async_remote_copy(
            src_ref=ev.at[pl.ds(first, size), pl.ds(0, part_y)],
            dst_ref=r.at[2, pl.ds(start, size)],
            send_sem=ds_sem.at[0],
            recv_sem=dr_sem.at[landing(AHEAD + k)],
            device_id={"deep": 0},
            device_id_type=pl.DeviceIdType.MESH,
        ).start()
        r[2, pl.ds(start, size)] = ev[pl.ds(first, size), part_y:]

    def send_north(picked):
        for c in picked:
            for other in evens if c in (3,) else norths:
                north_copy(c, other, n).start()
        for c in picked:
            u[rows(c, n), :] = wa[rows(c, n), :]

    split = sum(size for _, size in chunks[:early]) * north
    first.wait()
    for g in range(groups):
        loads[g].wait()
    for g in range(groups):
        along_x(g, 0, split)
    for table in tables:
        table.start()
    at = 0
    for source in (gx, gy, gz):
        span = pl.ds(at, source.shape[1])
        pltpu.make_async_copy(source, symbols.at[:, span], table_sem.at[3]).start()
        at += source.shape[1]
    pl.semaphore_wait(barrier, north - 1 + inner)
    if ahead:
        @pl.when(d == 2)
        def _():
            for copy in ahead_down():
                copy.start()

    send_north(range(early))
    if rounds:
        signal_beside(round_sem.at[0])
    if split < grid_x:
        for g in range(groups):
            along_x(g, split, grid_x - split)
        send_north(range(early, len(chunks)))

    for k in range(rounds - 1):
        pl.semaphore_wait(round_sem.at[k], inner)
        signal_beside(round_sem.at[k + 1])
    pltpu.make_async_copy(symbols, symbols, table_sem.at[3]).wait()
    at_y, at_z = grid_x, grid_x + grid_y
    spot = lax.broadcasted_iota(jnp.int32, (part_y, grid_y), 0) + d * part_y
    along = lax.broadcasted_iota(jnp.int32, (part_y, grid_y), 1)
    column = jnp.sum(jnp.where(spot == along, symbols[:, at_y:at_z], 0.0), axis=1, keepdims=True)
    plane = column + symbols[:, at_z:]
    spot = lax.broadcasted_iota(jnp.int32, (share_x, grid_x), 0) + n * share_x
    along = lax.broadcasted_iota(jnp.int32, (share_x, grid_x), 1)
    column = jnp.sum(jnp.where(spot == along, symbols[:, :at_y], 0.0), axis=1, keepdims=True)
    for i in range(share_x):
        symbol = column[i : i + 1] + plane
        fac[pl.ds(i * part_y, part_y), :] = (1.0 - 0.2 * symbol) / (1.0 + 0.2 * symbol)

    def along_y(blocks, base, size, i, pair, count):
        lines = jnp.concatenate(
            [
                jnp.concatenate(
                    [blocks[pl.ds(base + (s * size + i + k) * share_y, share_y), :] for s in range(north)],
                    axis=0,
                )
                for k in range(pair)
            ],
            axis=1,
        )
        high, low = halves(lines)
        return jnp.dot(
            hy[pl.ds(0, count), :],
            jnp.concatenate([high, low, high], axis=0),
            preferred_element_type=jnp.float32,
        )

    free = max(0, len(chunks) - HELD)
    def send_deep(c):
        if ahead and c in (AHEAD, AHEAD + 1):
            @pl.when((d != 2) | ~member[c - AHEAD])
            def _():
                for other in (deeps[0], *held):
                    deep_copy(c, other, d).start()

            deep_copy(c, deeps[1], d).start()
        elif held:
            far, side = deeps
            deep_copy(c, far, d).start()
            if c < free:
                if c == free - 1:
                    @pl.when(~patient)
                    def _():
                        deep_copy(c, held[0], d).start()
                        deep_copy(c, side, d).start()
                else:
                    deep_copy(c, held[0], d).start()
                    deep_copy(c, side, d).start()
            else:
                pl.when(inward)(lambda: deep_copy(c, side, d).start())
        else:
            for other in deeps:
                deep_copy(c, other, d).start()

    mine = pl.ds(pl.multiple_of(d * part_y, part_y), part_y)
    tables[0].wait()
    for c in range(len(chunks)):
        if c < len(chunks) - 1:
            north_landed(c)
        if c == 0 and rounds:
            pl.semaphore_wait(round_sem.at[rounds - 1], inner)
        start, size = chunks[c]
        for i in range(0, size, 2):
            pair = min(2, size - i)
            modes = along_y(u, start * north * share_y, size, i, pair, grid_y)
            for k in range(pair):
                v[start + i + k] = modes[:, k * lanes : (k + 1) * lanes]
        last = c == len(chunks) - 1
        send_deep(c)
        if held:
            for late in NEAR_AFTER.get(c, ()):
                pl.when(inward & ~(n == 0))(lambda late=late: deep_copy(late, held[0], d).start())
        if last and held:
            @pl.when(patient)
            def _():
                for other in (deeps[1], *held):
                    deep_copy(free - 1, other, d).start()

            @pl.when(~inward)
            def _():
                for late in range(free, len(chunks)):
                    for other in (*held, deeps[1]):
                        deep_copy(late, other, d).start()
        r[d, pl.ds(start, size)] = v[pl.ds(start, size), mine]
        if ahead and c == RELAY:
            @pl.when(d == 1)
            def _():
                every = ein.at[pl.ds(0, sent_ahead)]
                pltpu.make_async_copy(every, every, ahead_sem.at[0]).wait()
                for k in range(2):
                    for other in owners[k]:
                        @pl.when(n != other)
                        def _():
                            ahead_across(k, other, n).start()

                        @pl.when(n == other)
                        def _():
                            eu[ahead_block(k, other), :] = ein[ahead_block(k, other), :]

    if ahead:
        @pl.when(d == 1)
        def _():
            for mine, picked in cases:
                if picked:
                    def take():
                        size = sum(chunks[AHEAD + k][1] for k in picked)
                        every = eu.at[pl.ds(0, (north - 1) * size * share_y)]
                        pltpu.make_async_copy(every, every, ahead_sem.at[1]).wait()

                    pl.when(mine)(take)
            for k in range(2):
                pl.when(member[k])(lambda: ahead_modes(k))

    tables[1].wait()
    order = list(range(len(chunks)))
    if ahead:
        order = [RELAY, 0, AHEAD + 1, AHEAD, *range(RELAY + 1, len(chunks))]
    for c in order[:-1]:
        start, size = chunks[c]
        if not (merged and c == 0):
            deep_landed(c)
        if held:
            for late in NEAR_THEN.get(c, ()):
                pl.when(inward & (n == 0))(lambda late=late: deep_copy(late, held[0], d).start())
        parts = [r[s, pl.ds(*chunks[c])].reshape(size * part_y, lanes) for s in range(deep)]
        along_z(parts, fac[pl.ds(start * part_y, size * part_y), :], hz, out, start)
    start, size = chunks[order[-1]]
    factors[...] = fac[pl.ds(start * part_y, size * part_y), :]
    deep_landed(order[-1])
    final[...] = r[:, pl.ds(start, size)]

    def sent(semaphore, count):
        every = wa.at[pl.ds(0, count)]
        pltpu.make_async_copy(every, every, semaphore).wait()

    across, along = (north - 1) * share_x * share_y, (deep - 1) * share_x * part_y
    sent(ns_sem.at[0], across)
    if ahead:
        for mine, picked in cases:
            own = sum(chunks[AHEAD + k][1] for k in picked)
            over = sent_ahead - own * share_y + own * part_y
            down = sent_ahead - 2 * own * part_y
            pl.when((d == 1) & mine)(lambda: sent(ds_sem.at[0], along + over))
            pl.when((d == 2) & mine)(lambda: sent(ds_sem.at[0], along + down))
        pl.when(~inward)(lambda: sent(ds_sem.at[0], along))
    else:
        sent(ds_sem.at[0], along)


def along_z(parts, factor, hz, out, start):
    fields, _, part_y, grid_z = out.shape
    count, share_z = parts[0].shape[0], parts[0].shape[1] // fields
    size = count // part_y
    lines = [
        jnp.concatenate([p[:, f * share_z : (f + 1) * share_z] for p in parts], axis=1) for f in range(fields)
    ]
    if size <= 2:
        high, low = halves(jnp.concatenate(lines, axis=0))
        both = jnp.dot(
            jnp.concatenate([high, low], axis=0), hz[pl.ds(0, grid_z), :], preferred_element_type=jnp.float32
        )
        rest = jnp.dot(high, hz[pl.ds(2 * grid_z, grid_z), :], preferred_element_type=jnp.float32)
        modes = both[: fields * count] + both[fields * count :] + rest
        modes = [modes[f * count : (f + 1) * count] for f in range(fields)]
    else:
        modes = []
        for f in range(fields):
            high, low = halves(lines[f])
            modes.append(
                jnp.dot(jnp.concatenate([high, low, high], axis=1), hz[...], preferred_element_type=jnp.float32)
            )
    for f in range(fields):
        out[f, pl.ds(start, size)] = (modes[f] * factor).reshape(size, part_y, grid_z)


def finish(done, final, factors, hz, result, rest, sem):
    fields, share_x = done.shape[:2]
    deep, size, part_y, lanes = final.shape
    ahead = share_x - size
    bulk = pltpu.make_async_copy(done.at[:, pl.ds(0, ahead)], result.at[:, pl.ds(0, ahead)], sem.at[0])
    bulk.start()
    parts = [final[s].reshape(size * part_y, lanes) for s in range(deep)]
    along_z(parts, factors[...], hz, rest, 0)
    last = pltpu.make_async_copy(rest, result.at[:, pl.ds(ahead, size)], sem.at[1])
    last.start()
    bulk.wait()
    last.wait()


def local(north, deep, forcing, symbol_x, symbol_y, symbol_z):
    fields, grid_x, share_y, share_z = forcing.shape
    grid_y, grid_z = symbol_y.shape[0], symbol_z.shape[0]
    share_x, part_y = grid_x // north, grid_y // deep
    chunks = chunk_starts(share_x)
    lanes = fields * share_z

    modes = np.arange(grid_x).reshape(north, share_x)
    order = np.concatenate([modes[:, start : start + size].reshape(-1) for start, size in chunks])
    high, low = table_halves(transform_table(grid_x)[order])
    split = sum(size for _, size in chunks[:EARLY]) * north
    hx = np.concatenate(
        [
            np.block([[high[part], high[part]], [low[part], np.zeros_like(low[part])]])
            for part in (slice(0, split), slice(split, grid_x))
        ],
        axis=0,
    )
    high, low = table_halves(transform_table(grid_y))
    hy = np.concatenate([high, high, low], axis=1)
    high, low = table_halves(transform_table(grid_z))
    hz = np.concatenate([high, high, low], axis=0)

    groups, ahead = 1, deep == 4 and len(chunks) > RELAY
    most, more = (chunks[min(AHEAD + k, len(chunks) - 1)][1] for k in range(2))
    vmem = pl.BlockSpec(memory_space=pltpu.VMEM)
    buffers = [
        pltpu.VMEM((fields, share_y, share_z, grid_x), jnp.float32),
        pltpu.VMEM(hx.shape, jnp.bfloat16),
        pltpu.VMEM(hy.shape, jnp.bfloat16),
        pltpu.VMEM((grid_x * share_y, lanes), jnp.float32),
        pltpu.VMEM((grid_y * share_x, lanes), jnp.float32),
        pltpu.VMEM((share_x, grid_y, lanes), jnp.float32),
        pltpu.VMEM((deep, share_x, part_y, lanes), jnp.float32),
        pltpu.VMEM((share_x * part_y, grid_z), jnp.float32),
        pltpu.VMEM(((most + more) * north * share_y, lanes), jnp.float32),
        pltpu.VMEM(((most + more) * north * share_y, lanes), jnp.float32),
        pltpu.VMEM((most + more, 2 * part_y, lanes), jnp.float32),
    ]
    result = fields * share_x * part_y * grid_z
    held = sum(math.prod(b.shape) * jnp.dtype(b.dtype).itemsize for b in buffers)
    size = chunks[-1][1]
    done, final, factors, hz = pl.pallas_call(
        functools.partial(kernel, (north, deep, chunks, min(EARLY, len(chunks)))),
        out_shape=[
            pltpu.VMEM((fields, share_x, part_y, grid_z), jnp.float32),
            pltpu.VMEM((deep, size, part_y, lanes), jnp.float32),
            pltpu.VMEM((size * part_y, grid_z), jnp.float32),
            pltpu.VMEM(hz.shape, jnp.bfloat16),
        ],
        in_specs=[pl.BlockSpec(memory_space=pltpu.HBM)] * 7,
        out_specs=[vmem] * 4,
        scratch_shapes=[
            pltpu.VMEM((1, grid_x + grid_y + grid_z), jnp.float32),
            *buffers,
            pltpu.SemaphoreType.DMA((groups,)),
            pltpu.SemaphoreType.DMA((4,)),
            pltpu.SemaphoreType.DMA((1,)),
            pltpu.SemaphoreType.DMA((max(1, len(chunks) - 1),)),
            pltpu.SemaphoreType.DMA((1,)),
            pltpu.SemaphoreType.DMA((len(chunks) - 1 if ahead else len(chunks),)),
            pltpu.SemaphoreType.REGULAR((max(1, deep - 2),)),
            pltpu.SemaphoreType.DMA((2,)),
        ],
        compiler_params=pltpu.CompilerParams(
            collective_id=0, has_side_effects=True, vmem_limit_bytes=max(held + 2**23, 60 * 2**20 - 4 * result)
        ),
    )(
        forcing.transpose(0, 2, 3, 1),
        jnp.asarray(hx),
        jnp.asarray(hy),
        jnp.asarray(hz),
        symbol_x[None, :],
        symbol_y[None, :],
        symbol_z[None, :],
    )
    return pl.pallas_call(
        finish,
        out_shape=jax.ShapeDtypeStruct((fields, share_x, part_y, grid_z), jnp.float32),
        in_specs=[vmem] * 4,
        out_specs=pl.BlockSpec(memory_space=pltpu.HBM),
        scratch_shapes=[
            pltpu.VMEM((fields, size, part_y, grid_z), jnp.float32),
            pltpu.SemaphoreType.DMA((2,)),
        ],
        compiler_params=pltpu.CompilerParams(vmem_limit_bytes=2**24),
    )(*(pltpu.with_memory_space_constraint(held, pltpu.VMEM) for held in (done, final, factors, hz)))


def solution(mesh):
    placed = (P(None, None, "north", "deep"), P(), P(), P())
    return jax.shard_map(
        functools.partial(local, mesh.shape["north"], mesh.shape["deep"]),
        mesh=mesh,
        in_specs=placed,
        out_specs=P(None, "north", "deep", None),
        check_vma=False,
    )
```

```python
import functools
import math

import jax
import jax.numpy as jnp
import numpy as np
from jax import lax
from jax.experimental import pallas as pl
from jax.experimental.pallas import tpu as pltpu
from jax.sharding import PartitionSpec as P

CHUNKS = (1, 2, 1, 4, 4, 2, 2)
EARLY = 3
HELD = 3
AHEAD = 1
OWNERS = (((0, 8),), ((1, 2), (3, 4), (5, 6), (7, 8)))
RELAY = 3
NEAR_NOW = (0, 1, 2, 3)
NEAR_AFTER = {6: (4, 5, 6)}
NEAR_THEN = {3: (4, 5, 6)}


def transform_table(count):
    rank = np.arange(count)
    odd = (2 * rank[:, None] + 1) * (2 * rank[None, :] + 1) % (8 * count)
    return (np.cos(np.pi / (4 * count) * odd) * np.sqrt(2.0 / count)).astype(np.float32)


def chunk_starts(share):
    unit = max(1, share // sum(CHUNKS))
    found, start = [], 0
    for weight in CHUNKS:
        size = min(unit * weight, share - start)
        if size > 0:
            found.append((start, size))
        start += size
    if start < share:
        found.append((start, share - start))
    return tuple(found)


def halves(values):
    high = values.astype(jnp.bfloat16)
    low = (values - high.astype(jnp.float32)).astype(jnp.bfloat16)
    return high, low


def table_halves(table):
    high = table.astype(jnp.bfloat16)
    low = (table - high.astype(np.float32)).astype(jnp.bfloat16)
    return high, low


def partners(me, count):
    found = []
    for step in range(count - 1, 0, -1):
        if count & (count - 1):
            found.append(lax.rem(me + step, count))
            continue
        other = me
        for bit in range(count.bit_length() - 1):
            if step >> bit & 1:
                other = other + (1 - 2 * ((me // 2**bit) % 2)) * 2**bit
        found.append(other)
    return found


def kernel(
    sizes, forcing, tx, ty, tz, gx, gy, gz, out, final, factors, hz, symbols, xin, hx, hy, wa, u, v, r, fac, ein, eu, ev,
    in_sem, table_sem, ns_sem, nr_sem, ds_sem, dr_sem, round_sem, ahead_sem,
):
    north, deep, chunks, early = sizes
    fields, share_y, share_z, grid_x = forcing.shape
    share_x, part_y = out.shape[1], out.shape[2]
    grid_y, grid_z = v.shape[1], out.shape[3]
    lanes, rounds = fields * share_z, max(0, deep - 2)
    ahead = merged = deep == 4 and len(chunks) > RELAY
    if ahead:
        spans = [[(low, min(high, north)) for low, high in part if low < north] for part in OWNERS]
        owners = [[other for low, high in part for other in range(low, high)] for part in spans]
        sent_ahead = sum(len(owners[k]) * chunks[AHEAD + k][1] * share_y for k in range(2))
    n, d = lax.axis_index("north"), lax.axis_index("deep")
    norths, deeps = partners(n, north), partners(d, deep)
    evens = norths
    if north % 2 == 0 and north & (north - 1) == 0:
        chips = partners(n // 2, north // 2)
        evens = [2 * chip for chip in chips] + [2 * chip + 1 for chip in chips] + norths[-1:]
    held, inward, favoured = (), (d == 1) | (d == 2), n < 2
    if ahead:
        member = [functools.reduce(lambda a, b: a | b, [(n >= low) & (n < high) for low, high in part]) for part in spans]
        cases = (
            (member[0] & member[1], (0, 1)),
            (member[0] & ~member[1], (0,)),
            (~member[0] & member[1], (1,)),
            (~member[0] & ~member[1], ()),
        )
    patient = (d == 3) & favoured
    if deep == 4:
        far = jnp.where(d < 2, 3, 0)
        near, side = far + 1 - 2 * (far % 2), d + 1 - 2 * (d % 2)
        deeps, held = (far, side), (near,)

    first = pltpu.make_async_copy(tx, hx, table_sem.at[0])
    groups = in_sem.shape[0]
    per = share_y // groups
    loads = []
    for g in range(groups):
        part = (slice(None), pl.ds(g * per, per))
        loads.append(pltpu.make_async_copy(forcing.at[part], xin.at[part], in_sem.at[g]))
        loads[-1].start()
    first.start()

    barrier = pltpu.get_barrier_semaphore()
    inner = (d > 0).astype(jnp.int32) + (d < deep - 1).astype(jnp.int32)

    def signal_beside(semaphore):
        for other, there in ((d - 1, d > 0), (d + 1, d < deep - 1)):
            @pl.when(there)
            def _():
                pl.semaphore_signal(
                    semaphore, device_id={"deep": other}, device_id_type=pl.DeviceIdType.MESH
                )

    signal_beside(barrier)
    for other in norths:
        pl.semaphore_signal(barrier, device_id={"north": other}, device_id_type=pl.DeviceIdType.MESH)
    tables = [pltpu.make_async_copy(source, target, table_sem.at[k + 1]) for k, (source, target) in enumerate(((ty, hy), (tz, hz)))]
    pair = 2 if per % 2 == 0 else 1

    def along_x(g, start, count):
        for y in range(g * per, (g + 1) * per, pair):
            high, low = halves(
                jnp.concatenate([xin[f, y + k] for k in range(pair) for f in range(fields)], axis=0)
            )
            both = lax.dot_general(
                hx[pl.ds(2 * start, 2 * count), :],
                jnp.concatenate([high, low], axis=1),
                (((1,), (1,)), ((), ())),
                preferred_element_type=jnp.float32,
            )
            modes = both[:count] + both[count:]
            for k in range(pair):
                wa[pl.ds(start * share_y + y + k, count, stride=share_y), :] = modes[
                    :, k * lanes : (k + 1) * lanes
                ]

    def landing(c):
        return (c or RELAY) - 1 if merged else c

    def rows(c, other):
        start, size = chunks[c]
        at = (start * north + other * size) * share_y
        return pl.ds(pl.multiple_of(at, share_y), size * share_y)

    def north_copy(c, target, source):
        return pltpu.make_async_remote_copy(
            src_ref=wa.at[rows(c, target)],
            dst_ref=u.at[rows(c, source)],
            send_sem=ns_sem.at[0],
            recv_sem=nr_sem.at[min(c, len(chunks) - 2)],
            device_id={"north": target},
            device_id_type=pl.DeviceIdType.MESH,
        )

    def north_landed(c):
        size = sum(size for _, size in chunks[c:]) if c == len(chunks) - 2 else chunks[c][1]
        every = u.at[pl.ds(0, (north - 1) * size * share_y)]
        pltpu.make_async_copy(every, every, nr_sem.at[c]).wait()

    def deep_copy(c, target, source):
        return pltpu.make_async_remote_copy(
            src_ref=v.at[pl.ds(*chunks[c]), pl.ds(pl.multiple_of(target * part_y, part_y), part_y)],
            dst_ref=r.at[source, pl.ds(*chunks[c])],
            send_sem=ds_sem.at[0],
            recv_sem=dr_sem.at[landing(c)],
            device_id={"deep": target},
            device_id_type=pl.DeviceIdType.MESH,
        )

    def deep_landed(c):
        size = chunks[c][1] + (chunks[0][1] if merged and c == RELAY else 0)

        def take(count):
            every = r.at[pl.ds(0, count), pl.ds(0, size)]
            pltpu.make_async_copy(every, every, dr_sem.at[landing(c)]).wait()

        if ahead and c in (AHEAD, AHEAD + 1):
            own = (d == 1) & member[c - AHEAD]
            pl.when(own)(lambda: take(deep - 2))
            pl.when(~own)(lambda: take(deep - 1))
        else:
            take(deep - 1)

    def ahead_down():
        found = []
        for k in range(2):
            start, size = chunks[AHEAD + k]
            block, base = size * share_y, k * north * chunks[AHEAD][1] * share_y
            for low, high in spans[k]:
                part = pl.ds(low * block, (high - low) * block)
                found.append(
                    pltpu.make_async_remote_copy(
                        src_ref=wa.at[pl.ds(start * north * share_y + part.start, part.size)],
                        dst_ref=ein.at[pl.ds(base + part.start, part.size)],
                        send_sem=ds_sem.at[0],
                        recv_sem=ahead_sem.at[0],
                        device_id={"deep": 1},
                        device_id_type=pl.DeviceIdType.MESH,
                    )
                )
        return found

    def ahead_block(k, other):
        first, block = k * north * chunks[AHEAD][1] * share_y, chunks[AHEAD + k][1] * share_y
        return pl.ds(first + pl.multiple_of(other * block, block), block)

    def ahead_across(k, target, source):
        return pltpu.make_async_remote_copy(
            src_ref=ein.at[ahead_block(k, target)],
            dst_ref=eu.at[ahead_block(k, source)],
            send_sem=ds_sem.at[0],
            recv_sem=ahead_sem.at[1],
            device_id={"north": target},
            device_id_type=pl.DeviceIdType.MESH,
        )

    def ahead_modes(k):
        (start, size), first = chunks[AHEAD + k], k * chunks[AHEAD][1]
        for i in range(0, size, 2):
            pair = min(2, size - i)
            modes = along_y(eu, k * north * chunks[AHEAD][1] * share_y, size, i, pair, 2 * part_y)
            for j in range(pair):
                ev[first + i + j] = modes[:, j * lanes : (j + 1) * lanes]
        pltpu.make_async_remote_copy(
            src_ref=ev.at[pl.ds(first, size), pl.ds(0, part_y)],
            dst_ref=r.at[2, pl.ds(start, size)],
            send_sem=ds_sem.at[0],
            recv_sem=dr_sem.at[landing(AHEAD + k)],
            device_id={"deep": 0},
            device_id_type=pl.DeviceIdType.MESH,
        ).start()
        r[2, pl.ds(start, size)] = ev[pl.ds(first, size), part_y:]

    def send_north(picked):
        for c in picked:
            for other in evens if c in (3,) else norths:
                north_copy(c, other, n).start()
        for c in picked:
            u[rows(c, n), :] = wa[rows(c, n), :]

    split = sum(size for _, size in chunks[:early]) * north
    first.wait()
    for g in range(groups):
        loads[g].wait()
    for g in range(groups):
        along_x(g, 0, split)
    for table in tables:
        table.start()
    at = 0
    for source in (gx, gy, gz):
        span = pl.ds(at, source.shape[1])
        pltpu.make_async_copy(source, symbols.at[:, span], table_sem.at[3]).start()
        at += source.shape[1]
    pl.semaphore_wait(barrier, north - 1 + inner)
    if ahead:
        @pl.when(d == 2)
        def _():
            for copy in ahead_down():
                copy.start()

    send_north(range(early))
    if rounds:
        signal_beside(round_sem.at[0])
    if split < grid_x:
        for g in range(groups):
            along_x(g, split, grid_x - split)
        send_north(range(early, len(chunks)))

    for k in range(rounds - 1):
        pl.semaphore_wait(round_sem.at[k], inner)
        signal_beside(round_sem.at[k + 1])
    pltpu.make_async_copy(symbols, symbols, table_sem.at[3]).wait()
    at_y, at_z = grid_x, grid_x + grid_y
    spot = lax.broadcasted_iota(jnp.int32, (part_y, grid_y), 0) + d * part_y
    along = lax.broadcasted_iota(jnp.int32, (part_y, grid_y), 1)
    column = jnp.sum(jnp.where(spot == along, symbols[:, at_y:at_z], 0.0), axis=1, keepdims=True)
    plane = column + symbols[:, at_z:]
    spot = lax.broadcasted_iota(jnp.int32, (share_x, grid_x), 0) + n * share_x
    along = lax.broadcasted_iota(jnp.int32, (share_x, grid_x), 1)
    column = jnp.sum(jnp.where(spot == along, symbols[:, :at_y], 0.0), axis=1, keepdims=True)
    for i in range(share_x):
        symbol = column[i : i + 1] + plane
        fac[pl.ds(i * part_y, part_y), :] = (1.0 - 0.2 * symbol) / (1.0 + 0.2 * symbol)

    def along_y(blocks, base, size, i, pair, count):
        lines = jnp.concatenate(
            [
                jnp.concatenate(
                    [blocks[pl.ds(base + (s * size + i + k) * share_y, share_y), :] for s in range(north)],
                    axis=0,
                )
                for k in range(pair)
            ],
            axis=1,
        )
        high, low = halves(lines)
        return jnp.dot(
            hy[pl.ds(0, count), :],
            jnp.concatenate([high, low, high], axis=0),
            preferred_element_type=jnp.float32,
        )

    free = max(0, len(chunks) - HELD)
    def send_deep(c):
        if ahead and c in (AHEAD, AHEAD + 1):
            @pl.when((d != 2) | ~member[c - AHEAD])
            def _():
                for other in (deeps[0], *held):
                    deep_copy(c, other, d).start()

            deep_copy(c, deeps[1], d).start()
        elif held:
            far, side = deeps
            deep_copy(c, far, d).start()
            if c < free:
                if c == free - 1:
                    @pl.when(~patient)
                    def _():
                        deep_copy(c, held[0], d).start()
                        deep_copy(c, side, d).start()
                else:
                    deep_copy(c, held[0], d).start()
                    deep_copy(c, side, d).start()
            else:
                pl.when(inward)(lambda: deep_copy(c, side, d).start())
        else:
            for other in deeps:
                deep_copy(c, other, d).start()

    mine = pl.ds(pl.multiple_of(d * part_y, part_y), part_y)
    tables[0].wait()
    for c in range(len(chunks)):
        if c < len(chunks) - 1:
            north_landed(c)
        if c == 0 and rounds:
            pl.semaphore_wait(round_sem.at[rounds - 1], inner)
        start, size = chunks[c]
        for i in range(0, size, 2):
            pair = min(2, size - i)
            modes = along_y(u, start * north * share_y, size, i, pair, grid_y)
            for k in range(pair):
                v[start + i + k] = modes[:, k * lanes : (k + 1) * lanes]
        last = c == len(chunks) - 1
        send_deep(c)
        if held:
            for late in NEAR_AFTER.get(c, ()):
                pl.when(inward & ~(n == 0))(lambda late=late: deep_copy(late, held[0], d).start())
        if last and held:
            @pl.when(patient)
            def _():
                for other in (deeps[1], *held):
                    deep_copy(free - 1, other, d).start()

            @pl.when(~inward)
            def _():
                for late in range(free, len(chunks)):
                    for other in (*held, deeps[1]):
                        deep_copy(late, other, d).start()
        r[d, pl.ds(start, size)] = v[pl.ds(start, size), mine]
        if ahead and c == RELAY:
            @pl.when(d == 1)
            def _():
                every = ein.at[pl.ds(0, sent_ahead)]
                pltpu.make_async_copy(every, every, ahead_sem.at[0]).wait()
                for k in range(2):
                    for other in owners[k]:
                        @pl.when(n != other)
                        def _():
                            ahead_across(k, other, n).start()

                        @pl.when(n == other)
                        def _():
                            eu[ahead_block(k, other), :] = ein[ahead_block(k, other), :]

    if ahead:
        @pl.when(d == 1)
        def _():
            for mine, picked in cases:
                if picked:
                    def take():
                        size = sum(chunks[AHEAD + k][1] for k in picked)
                        every = eu.at[pl.ds(0, (north - 1) * size * share_y)]
                        pltpu.make_async_copy(every, every, ahead_sem.at[1]).wait()

                    pl.when(mine)(take)
            for k in range(2):
                pl.when(member[k])(lambda: ahead_modes(k))

    tables[1].wait()
    order = list(range(len(chunks)))
    if ahead:
        order = [RELAY, 0, AHEAD + 1, AHEAD, *range(RELAY + 1, len(chunks))]
    for c in order[:-1]:
        start, size = chunks[c]
        if not (merged and c == 0):
            deep_landed(c)
        if held:
            for late in NEAR_THEN.get(c, ()):
                pl.when(inward & (n == 0))(lambda late=late: deep_copy(late, held[0], d).start())
        parts = [r[s, pl.ds(*chunks[c])].reshape(size * part_y, lanes) for s in range(deep)]
        along_z(parts, fac[pl.ds(start * part_y, size * part_y), :], hz, out, start)
    start, size = chunks[order[-1]]
    factors[...] = fac[pl.ds(start * part_y, size * part_y), :]
    deep_landed(order[-1])
    final[...] = r[:, pl.ds(start, size)]

    def sent(semaphore, count):
        every = wa.at[pl.ds(0, count)]
        pltpu.make_async_copy(every, every, semaphore).wait()

    across, along = (north - 1) * share_x * share_y, (deep - 1) * share_x * part_y
    sent(ns_sem.at[0], across)
    if ahead:
        for mine, picked in cases:
            own = sum(chunks[AHEAD + k][1] for k in picked)
            over = sent_ahead - own * share_y + own * part_y
            down = sent_ahead - 2 * own * part_y
            pl.when((d == 1) & mine)(lambda: sent(ds_sem.at[0], along + over))
            pl.when((d == 2) & mine)(lambda: sent(ds_sem.at[0], along + down))
        pl.when(~inward)(lambda: sent(ds_sem.at[0], along))
    else:
        sent(ds_sem.at[0], along)


def along_z(parts, factor, hz, out, start):
    fields, _, part_y, grid_z = out.shape
    count, share_z = parts[0].shape[0], parts[0].shape[1] // fields
    size = count // part_y
    lines = [
        jnp.concatenate([p[:, f * share_z : (f + 1) * share_z] for p in parts], axis=1) for f in range(fields)
    ]
    if size <= 2:
        high, low = halves(jnp.concatenate(lines, axis=0))
        both = jnp.dot(
            jnp.concatenate([high, low], axis=0), hz[pl.ds(0, grid_z), :], preferred_element_type=jnp.float32
        )
        rest = jnp.dot(high, hz[pl.ds(2 * grid_z, grid_z), :], preferred_element_type=jnp.float32)
        modes = both[: fields * count] + both[fields * count :] + rest
        modes = [modes[f * count : (f + 1) * count] for f in range(fields)]
    else:
        modes = []
        for f in range(fields):
            high, low = halves(lines[f])
            modes.append(
                jnp.dot(jnp.concatenate([high, low, high], axis=1), hz[...], preferred_element_type=jnp.float32)
            )
    for f in range(fields):
        out[f, pl.ds(start, size)] = (modes[f] * factor).reshape(size, part_y, grid_z)


def finish(done, final, factors, hz, result, rest, sem):
    fields, share_x = done.shape[:2]
    deep, size, part_y, lanes = final.shape
    ahead = share_x - size
    bulk = [
        pltpu.make_async_copy(done.at[f, pl.ds(0, ahead)], result.at[f, pl.ds(0, ahead)], sem.at[f])
        for f in range(fields)
    ]
    for f in range(fields):
        bulk[f].start(priority=f % 2)
    parts = [final[s].reshape(size * part_y, lanes) for s in range(deep)]
    along_z(parts, factors[...], hz, rest, 0)
    last = pltpu.make_async_copy(rest, result.at[:, pl.ds(ahead, size)], sem.at[fields])
    last.start()
    for copy in bulk:
        copy.wait()
    last.wait()


def local(north, deep, forcing, symbol_x, symbol_y, symbol_z):
    fields, grid_x, share_y, share_z = forcing.shape
    grid_y, grid_z = symbol_y.shape[0], symbol_z.shape[0]
    share_x, part_y = grid_x // north, grid_y // deep
    chunks = chunk_starts(share_x)
    lanes = fields * share_z

    modes = np.arange(grid_x).reshape(north, share_x)
    order = np.concatenate([modes[:, start : start + size].reshape(-1) for start, size in chunks])
    high, low = table_halves(transform_table(grid_x)[order])
    split = sum(size for _, size in chunks[:EARLY]) * north
    hx = np.concatenate(
        [
            np.block([[high[part], high[part]], [low[part], np.zeros_like(low[part])]])
            for part in (slice(0, split), slice(split, grid_x))
        ],
        axis=0,
    )
    high, low = table_halves(transform_table(grid_y))
    hy = np.concatenate([high, high, low], axis=1)
    high, low = table_halves(transform_table(grid_z))
    hz = np.concatenate([high, high, low], axis=0)

    groups, ahead = 1, deep == 4 and len(chunks) > RELAY
    most, more = (chunks[min(AHEAD + k, len(chunks) - 1)][1] for k in range(2))
    vmem = pl.BlockSpec(memory_space=pltpu.VMEM)
    buffers = [
        pltpu.VMEM((fields, share_y, share_z, grid_x), jnp.float32),
        pltpu.VMEM(hx.shape, jnp.bfloat16),
        pltpu.VMEM(hy.shape, jnp.bfloat16),
        pltpu.VMEM((grid_x * share_y, lanes), jnp.float32),
        pltpu.VMEM((grid_y * share_x, lanes), jnp.float32),
        pltpu.VMEM((share_x, grid_y, lanes), jnp.float32),
        pltpu.VMEM((deep, share_x, part_y, lanes), jnp.float32),
        pltpu.VMEM((share_x * part_y, grid_z), jnp.float32),
        pltpu.VMEM(((most + more) * north * share_y, lanes), jnp.float32),
        pltpu.VMEM(((most + more) * north * share_y, lanes), jnp.float32),
        pltpu.VMEM((most + more, 2 * part_y, lanes), jnp.float32),
    ]
    result = fields * share_x * part_y * grid_z
    held = sum(math.prod(b.shape) * jnp.dtype(b.dtype).itemsize for b in buffers)
    size = chunks[-1][1]
    done, final, factors, hz = pl.pallas_call(
        functools.partial(kernel, (north, deep, chunks, min(EARLY, len(chunks)))),
        out_shape=[
            pltpu.VMEM((fields, share_x, part_y, grid_z), jnp.float32),
            pltpu.VMEM((deep, size, part_y, lanes), jnp.float32),
            pltpu.VMEM((size * part_y, grid_z), jnp.float32),
            pltpu.VMEM(hz.shape, jnp.bfloat16),
        ],
        in_specs=[pl.BlockSpec(memory_space=pltpu.HBM)] * 7,
        out_specs=[vmem] * 4,
        scratch_shapes=[
            pltpu.VMEM((1, grid_x + grid_y + grid_z), jnp.float32),
            *buffers,
            pltpu.SemaphoreType.DMA((groups,)),
            pltpu.SemaphoreType.DMA((4,)),
            pltpu.SemaphoreType.DMA((1,)),
            pltpu.SemaphoreType.DMA((max(1, len(chunks) - 1),)),
            pltpu.SemaphoreType.DMA((1,)),
            pltpu.SemaphoreType.DMA((len(chunks) - 1 if ahead else len(chunks),)),
            pltpu.SemaphoreType.REGULAR((max(1, deep - 2),)),
            pltpu.SemaphoreType.DMA((2,)),
        ],
        compiler_params=pltpu.CompilerParams(
            collective_id=0, has_side_effects=True, vmem_limit_bytes=max(held + 2**23, 60 * 2**20 - 4 * result)
        ),
    )(
        forcing.transpose(0, 2, 3, 1),
        jnp.asarray(hx),
        jnp.asarray(hy),
        jnp.asarray(hz),
        symbol_x[None, :],
        symbol_y[None, :],
        symbol_z[None, :],
    )
    return pl.pallas_call(
        finish,
        out_shape=jax.ShapeDtypeStruct((fields, share_x, part_y, grid_z), jnp.float32),
        in_specs=[vmem] * 4,
        out_specs=pl.BlockSpec(memory_space=pltpu.HBM),
        scratch_shapes=[
            pltpu.VMEM((fields, size, part_y, grid_z), jnp.float32),
            pltpu.SemaphoreType.DMA((fields + 1,)),
        ],
        compiler_params=pltpu.CompilerParams(vmem_limit_bytes=2**24),
    )(*(pltpu.with_memory_space_constraint(held, pltpu.VMEM) for held in (done, final, factors, hz)))


def solution(mesh):
    placed = (P(None, None, "north", "deep"), P(), P(), P())
    return jax.shard_map(
        functools.partial(local, mesh.shape["north"], mesh.shape["deep"]),
        mesh=mesh,
        in_specs=placed,
        out_specs=P(None, "north", "deep", None),
        check_vma=False,
    )
```
